32 devices in a mesh: seq: 16 (over z, x, core), head: 1, batch: 2 (over y).
Axes of the slice: x: 2, y: 2, z: 4, core: 2. Of those that a mesh axis runs over, the one named last changes fastest.
Arguments:
- queries: bfloat16 [2, 8192, 8, 8, 128], P('batch', 'seq', 'head'), may hold values from -160 to 160
- key_rows: bfloat16 [2, 8192, 8, 128], P('batch', 'seq'), may hold values from -6 to 6
- value_rows: bfloat16 [2, 8192, 8, 128], P('batch', 'seq'), may hold values from -6 to 6
- compressed: bfloat16 [2, 128, 8, 128], P('batch', 'seq'), may hold values from -6 to 6
- chosen: int32 [2, 128, 8, 16], P('batch', 'seq'), may hold values from 0 to 127, as said below
Outputs:
- block_scores: float32 [2, 128, 8, 128], P('batch', 'seq', 'head')
- attended: bfloat16 [2, 8192, 8, 8, 128], P('batch', 'seq', 'head')
The draws below stay inside these ranges and needn't reach their ends.
Inputs may be any that keep to these rules, and one draw needn't show every extreme that they name: `chosen`: every entry is at most its own tile number, and entry 0 of every row is the tile's own block. Over the tiles of one device of seq and one group, at most 2 different blocks of any other device are named, and every device after the first names exactly 2 blocks of the first device for each group.
All inputs are finite; a program needn't handle non-finite values.
Results may differ from the reference program's by a relative error of at most 0.008.
Values may be sent and summed in bfloat16 or wider, within the bound.
A program may use at most 128 MiB of HBM per device.

```python
import jax
import jax.numpy as jnp
from jax import lax

HPG = 8
G = 8
DH = 128
BLOCK = 64
TOPN = 16
BATCH = 2
SEQ_LEN = 8192
BLK_DEV = 8
NBLK = 128


def fields(key):
    key_one, key_two, key_three = jax.random.split(jax.random.fold_in(key, 71), 3)
    key_base = jnp.clip(jax.random.normal(key_one, (BATCH, SEQ_LEN, G, DH), jnp.float32), -5.0, 5.0)
    comp_base = jnp.clip(jax.random.normal(key_two, (BATCH, NBLK, G, DH), jnp.float32), -5.0, 5.0)
    query_base = jnp.clip(jax.random.normal(key_three, (BATCH, SEQ_LEN, HPG, G, DH), jnp.float32), -5.0, 5.0)
    return (query_base, key_base, comp_base)


def draw_queries(key, part):
    return fields(key)[0].astype(jnp.bfloat16)


def draw_key_rows(key, part):
    return fields(key)[1].astype(jnp.bfloat16)


def draw_compressed(key, part):
    return fields(key)[2].astype(jnp.bfloat16)


def draw_chosen(key, part):
    key_one, key_two, key_three = jax.random.split(jax.random.fold_in(key, 5), 3)
    shards = NBLK // BLK_DEV
    lower_pick = jax.random.randint(key_one, (BATCH, shards, G, shards), 0, BLK_DEV)
    upper_pick = (lower_pick + 1 + jax.random.randint(key_two, (BATCH, shards, G, shards), 0, BLK_DEV - 1)) % BLK_DEV
    offsets = jnp.arange(shards, dtype=jnp.int32) * BLK_DEV
    candidates = jnp.stack([lower_pick + offsets, upper_pick + offsets], axis=-1).reshape(BATCH, shards, G, shards * 2)
    tile_ids = jnp.arange(NBLK, dtype=jnp.int32)
    span_ids = tile_ids // BLK_DEV
    inner_ids = tile_ids % BLK_DEV
    remote_count = 2 * span_ids
    pool_size = remote_count + inner_ids + 1
    random_pointer = jax.random.randint(key_three, (BATCH, NBLK, G, TOPN), 0, pool_size[None, :, None, None])
    slot_ids = jnp.arange(TOPN, dtype=jnp.int32)[None, None, None, :]
    own_pointer = (remote_count + inner_ids)[None, :, None, None]
    sink_pointer = (inner_ids % 2)[None, :, None, None]
    has_remote = (span_ids > 0)[None, :, None, None]
    pointer = jnp.where(slot_ids == 0, own_pointer, jnp.where((slot_ids == 1) & has_remote, sink_pointer, random_pointer))
    tile_candidates = candidates[:, span_ids]
    remote_ids = jnp.take_along_axis(tile_candidates, jnp.clip(pointer, 0, shards * 2 - 1), axis=-1)
    local_ids = (span_ids * BLK_DEV - remote_count)[None, :, None, None] + pointer
    return jnp.where(pointer < remote_count[None, :, None, None], remote_ids, local_ids).astype(jnp.int32)


def levels(key, extent, pieces, least, top_value):
    gain = 1.0
    for position, parts in pieces:
        draws = jax.random.uniform(jax.random.fold_in(jax.random.fold_in(key, 6), position), (parts,), jnp.float32, least / len(pieces), top_value / len(pieces))
        gain = gain * jnp.repeat(jnp.exp(draws), extent[position] // parts).reshape((-1,) + (1,) * (len(extent) - 1 - position))
    return gain


def gaussian(key, shape, scale, most, pieces=(), kind=jnp.bfloat16):
    result = scale * jax.random.normal(key, shape, jnp.float32)
    if pieces:
        result = result * levels(key, shape, pieces, -0.22, 0.18)
    return jnp.clip(result, -most, most).astype(kind)


def setup_inputs(seed: int = 0) -> dict:
    key_of = jax.random.split(jax.random.key(seed), 6)
    return {
        "queries": draw_queries(jax.random.fold_in(key_of[5], 71), 0),
        "key_rows": draw_key_rows(jax.random.fold_in(key_of[5], 71), 0),
        "value_rows": gaussian(key_of[2], (BATCH, SEQ_LEN, G, DH), 1.0, 6.0, ((0, 2), (1, 16))),
        "compressed": draw_compressed(jax.random.fold_in(key_of[5], 71), 0),
        "chosen": draw_chosen(jax.random.fold_in(key_of[5], 71), 0),
    }


def softmax_parts(scores):
    row_top = jnp.max(scores, axis=-1, keepdims=True)
    weights = jnp.exp(scores - row_top)
    return weights, jnp.sum(weights, axis=-1, keepdims=True)


def one_sequence(inputs):
    query_seq, key_seq, value_seq, compressed_seq, chosen_seq = inputs
    score_scale = DH ** -0.5
    tile_step = 2
    rounds = NBLK // tile_step
    key_blocks = key_seq.reshape(NBLK, BLOCK, G, DH)
    value_blocks = value_seq.reshape(NBLK, BLOCK, G, DH)
    all_blocks = jnp.arange(NBLK, dtype=jnp.int32)
    group_ids = jnp.arange(G, dtype=jnp.int32)[None, :, None]
    comp_wide = compressed_seq.astype(jnp.float32)

    def per_round(round_in):
        query_part, pick_part, round_id = round_in
        query_pos = round_id * (tile_step * BLOCK) + jnp.arange(tile_step * BLOCK, dtype=jnp.int32)
        query_wide = query_part.astype(jnp.float32)
        logits = jnp.einsum("qhgd,ngd->qhgn", query_wide, comp_wide) * score_scale
        seen = all_blocks[None, :] <= (query_pos // BLOCK)[:, None]
        logits = jnp.where(seen[:, None, None, :], logits, -jnp.inf)
        weights, totals = softmax_parts(logits)
        probability = weights / totals
        pooled = jnp.sum(probability.reshape(tile_step, BLOCK, HPG, G, NBLK), axis=(1, 2))
        tile_ids = round_id * tile_step + jnp.arange(tile_step, dtype=jnp.int32)
        factor = (tile_ids + 1).astype(jnp.float32) / (BLOCK * HPG)
        scores_out = pooled * factor[:, None, None]
        key_sel = key_blocks[pick_part, :, group_ids, :].reshape(tile_step, G, TOPN * BLOCK, DH)
        value_sel = value_blocks[pick_part, :, group_ids, :].reshape(tile_step, G, TOPN * BLOCK, DH)
        key_pos = (pick_part[..., None] * BLOCK + jnp.arange(BLOCK, dtype=jnp.int32)).reshape(tile_step, G, TOPN * BLOCK)
        query_tiles = query_wide.reshape(tile_step, BLOCK, HPG, G, DH)
        scores = jnp.einsum("tqhgd,tgkd->tghqk", query_tiles, key_sel.astype(jnp.float32)) * score_scale
        tile_pos = query_pos.reshape(tile_step, BLOCK)
        visible = key_pos[:, :, None, None, :] <= tile_pos[:, None, None, :, None]
        scores = jnp.where(visible, scores, -jnp.inf)
        weights, totals = softmax_parts(scores)
        rounded = weights.astype(jnp.bfloat16)
        mixed = jnp.einsum("tghqk,tgkd->tqhgd", rounded.astype(jnp.float32), value_sel.astype(jnp.float32))
        attended = (mixed / jnp.transpose(totals, (0, 3, 2, 1, 4))).astype(jnp.bfloat16)
        return scores_out, attended.reshape(tile_step * BLOCK, HPG, G, DH)

    round_ids = jnp.arange(rounds, dtype=jnp.int32)
    scores_out, attended = lax.map(per_round, (query_seq.reshape(rounds, tile_step * BLOCK, HPG, G, DH), chosen_seq.reshape(rounds, tile_step, G, TOPN), round_ids))
    return scores_out.reshape(NBLK, G, NBLK), attended.reshape(SEQ_LEN, HPG, G, DH)


def reference(queries, key_rows, value_rows, compressed, chosen):
    block_scores, attended = lax.map(one_sequence, (queries, key_rows, value_rows, compressed, chosen))
    return block_scores, attended
```

```python
import functools
import math

import jax
import jax.numpy as jnp
from jax import lax
from jax.experimental import pallas as pl
from jax.experimental.pallas import tpu as pltpu
from jax.sharding import PartitionSpec as P

HPG = 8
BLOCK = 64
TOPN = 16
CAP = 2
COLS = 2
CORES = 2
MESH = pl.DeviceIdType.MESH


def mega(
    shape,
    slot_ref,
    pick_ref,
    wanted_ref,
    own_ref,
    query_ref,
    out_ref,
    pooled_ref,
    column,
    peer_out,
    peer_in,
    cur,
    comp,
    queries,
    mixed_out,
    picked,
    peer_wanted,
    peer_wanted_s,
    up_send,
    up_recv,
    sib_send,
    sib_recv,
    peer_send,
    peer_recv,
    own_sem,
    query_sem,
    out_sem,
    misc_sem,
):
    levels, groups, blk_dev, heads_local, block_len, head_width = shape
    rows = block_len * heads_local
    tokens = blk_dev * block_len
    per_level = COLS * CORES
    slots_col = levels * CORES * blk_dev
    picks = CORES * CAP

    rank = lax.axis_index("seq")
    core = lax.rem(rank, CORES)
    col = lax.rem(rank // CORES, COLS)
    level = rank // per_level
    sibling = rank + 1 - 2 * core
    peer = rank + CORES * (1 - 2 * col)
    above = rank + per_level
    below = rank - per_level
    has_above = level < levels - 1
    has_below = level > 0

    barrier = pltpu.get_barrier_semaphore()
    for other in (sibling, peer):
        pl.semaphore_signal(barrier, inc=1, device_id={"seq": other}, device_id_type=MESH)

    @pl.when(has_above)
    def _():
        pl.semaphore_signal(barrier, inc=1, device_id={"seq": above}, device_id_type=MESH)

    @pl.when(has_below)
    def _():
        pl.semaphore_signal(barrier, inc=1, device_id={"seq": below}, device_id_type=MESH)

    def own_copy(g):
        return pltpu.make_async_copy(own_ref.at[g], column.at[level, core, g], own_sem.at[g])

    def query_copy(g):
        return pltpu.make_async_copy(query_ref.at[g], queries.at[g], query_sem.at[g])

    def out_copy(g):
        return pltpu.make_async_copy(mixed_out.at[g], out_ref.at[g], out_sem.at[g])

    def up(l, g):
        part = column.at[l, core, g]
        return pltpu.make_async_remote_copy(
            part, part, up_send.at[l, g], up_recv.at[l, g], device_id={"seq": above}, device_id_type=MESH
        )

    def aside(l, g, owner):
        part = column.at[l, owner, g]
        return pltpu.make_async_remote_copy(
            part, part, sib_send.at[l, g], sib_recv.at[l, g], device_id={"seq": sibling}, device_id_type=MESH
        )

    def across(l, g):
        return pltpu.make_async_remote_copy(
            peer_out.at[g, l],
            peer_in.at[g, l],
            peer_send.at[l, g],
            peer_recv.at[l, g],
            device_id={"seq": peer},
            device_id_type=MESH,
        )

    wanted_copy = pltpu.make_async_remote_copy(
        wanted_ref, peer_wanted, misc_sem.at[0], misc_sem.at[1], device_id={"seq": peer}, device_id_type=MESH
    )

    def loop(n, body):
        def step(i, carry):
            body(i)
            return carry

        lax.fori_loop(0, n, step, 0)

    loop(groups, lambda g: own_copy(g).start())
    loop(groups, lambda g: query_copy(g).start())
    comp[...] = jnp.zeros_like(comp)

    count = 2 + has_above.astype(jnp.int32) + has_below.astype(jnp.int32)
    pl.semaphore_wait(barrier, count)
    wanted_copy.start()

    def pass_on(l, g):
        @pl.when(has_above)
        def _():
            up(l, g).start()

        aside(l, g, core).start()

    def forward(g):
        own_copy(g).wait()
        pass_on(level, g)

        def relay(i):
            l = level - 1 - i
            up(l, g).wait_recv()
            pass_on(l, g)

        loop(level, relay)

    def take_column(g):
        half = lax.rem(g, 2)

        def body(l):
            aside(l, g, 1 - core).wait_recv()
            for c in range(CORES):
                first = (l * CORES + c) * blk_dev
                for b in range(blk_dev):
                    cur[half, first + b] = column[l, c, g, b * block_len : (b + 1) * block_len]
                keys = column[l, c, g, tokens : tokens + blk_dev, :head_width]
                comp[half, (l * COLS + col) * CORES + c] = keys.astype(jnp.float32)

        loop(level + 1, body)

    def serve_peer(g):
        half = lax.rem(g, 2)

        def body(l):
            for c in range(CORES):
                source = (l * COLS + col) * CORES + c
                for k in range(CAP):
                    index = peer_wanted_s[g, source * CAP + k]
                    place = (c * CAP + k) * block_len
                    peer_out[g, l, place : place + block_len] = cur[half, (l * CORES + c) * blk_dev + index]
            first = (l * COLS + col) * CORES
            keys = comp[half, pl.ds(first, CORES)].reshape(CORES * blk_dev, head_width)
            keys = keys.astype(jnp.bfloat16)
            peer_out[g, l, picks * block_len :] = jnp.concatenate([keys, keys], axis=1)
            across(l, g).start()

        loop(level + 1, body)

    def take_peer(g):
        half = lax.rem(g, 2)

        def body(l):
            across(l, g).wait_recv()
            for k in range(picks):
                cur[half, slots_col + l * picks + k] = peer_in[g, l, k * block_len : (k + 1) * block_len]
            keys = peer_in[g, l, picks * block_len :, :head_width].astype(jnp.float32)
            first = (l * COLS + 1 - col) * CORES
            comp[half, pl.ds(first, CORES)] = keys.reshape(CORES, blk_dev, head_width)

        loop(level + 1, body)

    factor = math.log2(math.e) * head_width ** (-0.5)
    part = min(rows, 256)
    keys_all = TOPN * block_len
    nblk = levels * per_level * blk_dev

    def compute(g):
        half = lax.rem(g, 2)
        query_copy(g).wait()
        key_position = lax.broadcasted_iota(jnp.int32, (1, keys_all), 1)
        within = key_position % block_len
        block_place = key_position // block_len
        block_number = lax.broadcasted_iota(jnp.int32, (1, nblk), 1)

        def tile_body(t):
            tile_number = rank * blk_dev + t
            limit = jnp.full((1, keys_all), -1, jnp.int32)
            for place in range(TOPN):
                picked[place * block_len : (place + 1) * block_len] = cur[half, slot_ref[t, g, place]]
                is_own = pick_ref[t, g, place] == tile_number
                limit = jnp.where((block_place == place) & is_own, within, limit)
            summary = comp[half].reshape(nblk, head_width).astype(jnp.bfloat16)
            pooled = jnp.zeros((1, nblk), jnp.float32)
            for start in range(0, rows, part):
                query = queries[g, t, start : start + part]
                logits = lax.dot_general(
                    query, summary, (((1,), (1,)), ((), ())), preferred_element_type=jnp.float32
                )
                logits = jnp.where(block_number <= tile_number, logits, -jnp.inf)
                top = jnp.max(logits, axis=-1, keepdims=True)
                weights = jnp.exp2((logits - top) * factor)
                totals = jnp.sum(weights, axis=-1, keepdims=True)
                pooled += jnp.sum(weights / totals, axis=0, keepdims=True)

                scores = lax.dot_general(
                    query, picked[:, :head_width], (((1,), (1,)), ((), ())), preferred_element_type=jnp.float32
                )
                token = (start + lax.broadcasted_iota(jnp.int32, (part, 1), 0)) // heads_local
                scores = jnp.where(limit <= token, scores, -jnp.inf)
                row_top = jnp.max(scores, axis=-1, keepdims=True)
                weights = jnp.exp2((scores - row_top) * factor)
                totals = jnp.sum(weights, axis=-1, keepdims=True)
                mixed = jnp.dot(
                    weights.astype(jnp.bfloat16), picked[:, head_width:], preferred_element_type=jnp.float32
                )
                mixed_out[g, t, start : start + part] = (mixed / totals).astype(jnp.bfloat16)
            pooled_ref[pl.ds(t * groups + g, 1), :] = pooled

        loop(blk_dev, tile_body)
        out_copy(g).start()

    forward(0)
    wanted_copy.wait_recv()
    local = pltpu.make_async_copy(peer_wanted, peer_wanted_s, misc_sem.at[2])
    local.start()
    local.wait()

    def main(g):
        @pl.when(g + 1 < groups)
        def _():
            forward(g + 1)

        take_column(g)
        serve_peer(g)

        @pl.when(g > 0)
        def _():
            take_peer(g - 1)
            compute(g - 1)

    loop(groups, main)
    take_peer(groups - 1)
    compute(groups - 1)

    wanted_copy.wait_send()

    def drain(g):
        def body(l):
            @pl.when(has_above)
            def _():
                up(l, g).wait_send()

            aside(l, g, core).wait_send()
            across(l, g).wait_send()

        loop(level + 1, body)
        out_copy(g).wait()

    loop(groups, drain)


def local(queries, key_rows, value_rows, compressed, chosen):
    _, tok_rows, heads_local, groups, head_width = queries.shape
    block_len = BLOCK
    shards = lax.axis_size("seq")
    seq_rank = lax.axis_index("seq")
    blk_dev = tok_rows // block_len
    nblk = blk_dev * shards
    levels = shards // (COLS * CORES)
    rows = block_len * heads_local

    pick_rows = chosen[0]
    all_blocks = jnp.arange(nblk, dtype=jnp.int32)
    onehot = pick_rows[..., None] == all_blocks
    needed = jnp.any(onehot, axis=(0, 2))
    owner_of = all_blocks // blk_dev
    own_col = (seq_rank // CORES) % COLS
    in_column = (owner_of // CORES) % COLS == own_col
    needed_grid = needed.reshape(groups, shards, blk_dev).astype(jnp.int32)
    rank_in = jnp.cumsum(needed_grid, axis=2) - needed_grid
    places = jnp.arange(CAP, dtype=jnp.int32)
    within = jnp.arange(blk_dev, dtype=jnp.int32)
    matched = (needed_grid[..., None] == 1) & (rank_in[..., None] == places)
    wanted = jnp.sum(jnp.where(matched, within[:, None], 0), axis=2)
    wanted = wanted.reshape(groups, shards * CAP)
    wanted = jnp.pad(wanted, ((0, 0), (0, -shards * CAP % 128)))
    pair = owner_of // (COLS * CORES) * CORES + owner_of % CORES
    slot_column = pair * blk_dev + all_blocks % blk_dev
    slot_peer = levels * CORES * blk_dev + pair[None, :] * CAP + rank_in.reshape(groups, nblk)
    slot_of = jnp.where(in_column[None, :], slot_column[None, :], slot_peer)
    pool_index = jnp.sum(jnp.where(onehot, slot_of[None, :, None, :], 0), axis=3)

    key_local = key_rows[0].reshape(tok_rows, groups, head_width)
    value_local = value_rows[0].reshape(tok_rows, groups, head_width)
    own_rows = jnp.transpose(jnp.concatenate([key_local, value_local], axis=-1), (1, 0, 2))
    keys = jnp.transpose(compressed[0], (1, 0, 2))
    pad_rows = 16 * -(-blk_dev // 16)
    extra = jnp.pad(keys, ((0, 0), (0, pad_rows - blk_dev), (0, head_width)))
    own_rows = jnp.concatenate([own_rows, extra], axis=1)
    query_tiles = jnp.transpose(
        queries[0].reshape(blk_dev, rows, groups, head_width), (2, 0, 1, 3)
    )
    shape = (levels, groups, blk_dev, heads_local, block_len, head_width)
    wide = 2 * head_width
    chunk = tok_rows + pad_rows
    served = CORES * CAP * block_len + CORES * blk_dev
    dma = pltpu.SemaphoreType.DMA
    smem = pl.BlockSpec(memory_space=pltpu.SMEM)
    vmem = pl.BlockSpec(memory_space=pltpu.VMEM)
    anyspace = pl.BlockSpec(memory_space=pl.ANY)
    slots = levels * CORES * (blk_dev + CAP)
    bf16 = jnp.bfloat16
    attended, pooled = pl.pallas_call(
        functools.partial(mega, shape),
        in_specs=[smem, smem, vmem, anyspace, anyspace],
        out_specs=[anyspace, vmem],
        out_shape=[
            jax.ShapeDtypeStruct((groups, blk_dev, rows, head_width), bf16),
            jax.ShapeDtypeStruct((blk_dev * groups, nblk), jnp.float32),
        ],
        scratch_shapes=[
            pltpu.VMEM((levels, CORES, groups, chunk, wide), bf16),
            pltpu.VMEM((groups, levels, served, wide), bf16),
            pltpu.VMEM((groups, levels, served, wide), bf16),
            pltpu.VMEM((2, slots, block_len, wide), bf16),
            pltpu.VMEM((2, shards, blk_dev, head_width), jnp.float32),
            pltpu.VMEM((groups, blk_dev, rows, head_width), bf16),
            pltpu.VMEM((groups, blk_dev, rows, head_width), bf16),
            pltpu.VMEM((TOPN * block_len, wide), bf16),
            pltpu.VMEM(wanted.shape, jnp.int32),
            pltpu.SMEM(wanted.shape, jnp.int32),
        ]
        + [dma((levels, groups))] * 6
        + [dma((groups,))] * 3
        + [dma((3,))],
        compiler_params=pltpu.CompilerParams(
            collective_id=0, has_side_effects=True, vmem_limit_bytes=67043328
        ),
    )(pool_index, pick_rows, wanted, own_rows, query_tiles)
    pooled = pooled.reshape(1, blk_dev, groups, nblk)
    shared = lax.psum_scatter(pooled, "head", scatter_dimension=2, tiled=True)
    tile_ids = seq_rank * blk_dev + jnp.arange(blk_dev, dtype=jnp.int32)
    factor = (tile_ids + 1).astype(jnp.float32) / (block_len * HPG)
    block_scores = shared * factor[None, :, None, None]
    attended = jnp.transpose(attended, (1, 2, 0, 3))
    attended = attended.reshape(1, tok_rows, heads_local, groups, head_width)
    return (block_scores, attended)


def solution(mesh):
    placed = (
        P("batch", "seq", "head", None, None),
        P("batch", "seq", None, None),
        P("batch", "seq", None, None),
        P("batch", "seq", None, None),
        P("batch", "seq", None, None),
    )
    return jax.shard_map(
        local,
        mesh=mesh,
        in_specs=placed,
        out_specs=(P("batch", "seq", "head", None), P("batch", "seq", "head", None, None)),
        check_vma=False,
    )
```

```python
import functools
import math

import jax
import jax.numpy as jnp
from jax import lax
from jax.experimental import pallas as pl
from jax.experimental.pallas import tpu as pltpu
from jax.sharding import PartitionSpec as P

HPG = 8
BLOCK = 64
TOPN = 16
CAP = 2
COLS = 2
CORES = 2
MESH = pl.DeviceIdType.MESH


def mega(
    shape,
    pick_ref,
    chosen_ref,
    summary_ref,
    key_ref,
    value_ref,
    query_ref,
    out_ref,
    pooled_ref,
    column,
    peer_out,
    peer_in,
    cur,
    summaries,
    summaries_wide,
    queries,
    wide_out,
    stage,
    rows_stage,
    key_part,
    value_part,
    scores_part,
    token_hot,
    mask_bank,
    slot_map,
    slot_map_s,
    wanted,
    peer_wanted,
    peer_wanted_s,
    up_send,
    up_recv,
    sib_send,
    sib_recv,
    peer_send,
    peer_recv,
    key_send,
    key_recv,
    stage_sem,
    misc_sem,
):
    levels, groups, blk_dev, heads_local, block_len, head_width = shape
    rows = block_len * heads_local
    per_level = COLS * CORES
    slots_col = levels * CORES * blk_dev
    picks = CORES * CAP
    f32, bf16 = jnp.float32, jnp.bfloat16

    rank = lax.axis_index("seq")
    core = lax.rem(rank, CORES)
    col = lax.rem(rank // CORES, COLS)
    level = rank // per_level
    sibling = rank + 1 - 2 * core
    peer = rank + CORES * (1 - 2 * col)
    above = rank + per_level
    has_above = level < levels - 1

    def loop(n, body, start=0):
        def step(i, carry):
            body(i)
            return carry

        lax.fori_loop(start, n, step, 0)

    barrier = pltpu.get_barrier_semaphore()
    for other in (sibling, peer):
        pl.semaphore_signal(barrier, inc=1, device_id={"seq": other}, device_id_type=MESH)
    for step in range(1, levels):
        other = lax.rem(rank + step * per_level, levels * per_level)
        pl.semaphore_signal(barrier, inc=1, device_id={"seq": other}, device_id_type=MESH)

    def query_copy(t):
        half = lax.rem(t, 2)
        return pltpu.make_async_copy(query_ref.at[t], stage.at[half], stage_sem.at[half])

    def out_copy(t):
        half = lax.rem(t, 2)
        return pltpu.make_async_copy(stage.at[half], out_ref.at[t], stage_sem.at[half])

    def remote(src, dst, send, recv, device):
        return pltpu.make_async_remote_copy(
            src, dst, send, recv, device_id={"seq": device}, device_id_type=MESH
        )

    def up(l, g):
        part = column.at[l, core, g]
        return remote(part, part, up_send.at[l, g], up_recv.at[l, g], above)

    def aside(l, g, owner):
        part = column.at[l, owner, g]
        return remote(part, part, sib_send.at[l, g], sib_recv.at[l, g], sibling)

    def across(l, g):
        return remote(peer_out.at[g, l], peer_in.at[g, l], peer_send.at[l, g], peer_recv.at[l, g], peer)

    def keys_up(l, source):
        part = summaries.at[source, col, core]
        return remote(part, part, key_send.at[0, l], key_recv.at[0, source], rank + (l - level) * per_level)

    def keys_aside(l, owner):
        part = summaries.at[l, col, owner]
        return remote(part, part, key_send.at[1, l], key_recv.at[1, l], sibling)

    def keys_across(l, owner):
        part = summaries.at[l, owner]
        return remote(part, part, key_send.at[2, l], key_recv.at[2, l], peer)

    wanted_copy = remote(wanted, peer_wanted, misc_sem.at[0], misc_sem.at[1], peer)
    slots_copy = pltpu.make_async_copy(slot_map, slot_map_s, misc_sem.at[2])
    loads = [
        pltpu.make_async_copy(key_ref, rows_stage.at[0], misc_sem.at[4]),
        pltpu.make_async_copy(value_ref, rows_stage.at[1], misc_sem.at[5]),
    ]
    for load in loads:
        load.start()
    query_copy(0).start()

    nblk = levels * per_level * blk_dev
    number = lax.broadcasted_iota(jnp.int32, (groups, nblk), 1)
    named = jnp.zeros((groups, nblk), jnp.int32)
    for t in range(blk_dev):
        picks_here = chosen_ref[t]
        for place in range(TOPN):
            named = jnp.where(picks_here[:, place : place + 1] == number, 1, named)
    inside = lax.rem(number, blk_dev)
    order = named
    step = 1
    while step < blk_dev:
        order = order + jnp.where(inside >= step, pltpu.roll(order, step, 1), 0)
        step *= 2
    order = order - named
    for k in range(CAP):
        found = jnp.where((named == 1) & (order == k), inside, 0)
        step = 1
        while step < blk_dev:
            found = found + pltpu.roll(found, nblk - step, 1)
            step *= 2
        wanted[k] = found
    device = number // blk_dev
    pair = device // per_level * CORES + lax.rem(device, CORES)
    in_column = lax.rem(device // CORES, COLS) == col
    slot_map[...] = jnp.where(in_column, pair * blk_dev + inside, slots_col + pair * CAP + order)

    own_summary = jnp.swapaxes(summary_ref[...].astype(f32), 0, 1)
    own_summary = own_summary.reshape(groups * blk_dev, head_width).astype(bf16)
    summaries[level, col, core] = own_summary
    row_token = lax.broadcasted_iota(jnp.int32, (rows, head_width), 0) // heads_local
    row_lane = lax.broadcasted_iota(jnp.int32, (rows, head_width), 1)
    token_hot[...] = jnp.where(row_token == row_lane, 1.0, 0.0).astype(bf16)
    key_place = lax.broadcasted_iota(jnp.int32, (block_len, head_width), 0)
    key_lane = lax.broadcasted_iota(jnp.int32, (block_len, head_width), 1)
    mask_bank[0] = jnp.zeros((block_len, head_width), bf16)
    mask_bank[1] = jnp.where(key_place > key_lane, -1e30, 0.0).astype(bf16)
    value_part[:, head_width:] = jnp.ones((TOPN * block_len, head_width), bf16)
    summaries_wide[...] = jnp.zeros_like(summaries_wide)
    for kind in range(2):
        loads[kind].wait()

        def split(r, kind=kind):
            here = pl.ds(pl.multiple_of(r * block_len, block_len), block_len)
            apart = jnp.swapaxes(rows_stage[kind, here].astype(f32), 0, 1).astype(bf16)
            for g in range(groups):
                column[level, core, g, here, kind * head_width : (kind + 1) * head_width] = apart[g]

        loop(blk_dev, split)
    slots_copy.start()
    pl.semaphore_wait(barrier, levels + 1)

    loop(levels, lambda l: keys_up(l, level).start(), level + 1)
    keys_aside(level, core).start()
    wanted_copy.start()

    def send_own(g):
        @pl.when(has_above)
        def _():
            up(level, g).start()

    lead = 3
    for g in range(min(lead, groups - 1)):
        send_own(g)
    loop(groups, lambda g: aside(level, g, core).start())

    def spread(t):
        query_copy(t).wait()

        @pl.when(t + 1 < blk_dev)
        def _():
            query_copy(t + 1).start()

        half = lax.rem(t, 2)
        wide_out[t] = stage[half].astype(f32).reshape(rows * groups, head_width)
        for g in range(groups):
            queries[g, t] = wide_out[t, pl.ds(g, rows, stride=groups)].astype(bf16)

    loop(blk_dev, spread)

    def relay_keys(l):
        keys_up(l, l).wait_recv()
        keys_aside(l, core).start()

    def pair_keys(l):
        keys_aside(l, 1 - core).wait_recv()
        keys_across(l, col).start()

    def widen_keys(l):
        keys_across(l, 1 - col).wait_recv()
        for x in range(COLS):
            for c in range(CORES):
                summaries_wide[(l * COLS + x) * CORES + c] = summaries[l, x, c].astype(f32)

    loop(level, relay_keys)
    loop(level + 1, pair_keys)
    wanted_copy.wait_recv()
    local_wanted = pltpu.make_async_copy(peer_wanted, peer_wanted_s, misc_sem.at[3])
    local_wanted.start()
    local_wanted.wait()
    slots_copy.wait()
    loop(level + 1, widen_keys)

    def relay(g, l):
        up(l, g).wait_recv()

        @pl.when(has_above)
        def _():
            up(l, g).start()

        aside(l, g, core).start()

    def take(g, l):
        half = lax.rem(g, 2)
        aside(l, g, 1 - core).wait_recv()
        for c in range(CORES):
            first = (l * CORES + c) * blk_dev
            for b in range(blk_dev):
                cur[half, first + b] = column[l, c, g, b * block_len : (b + 1) * block_len]
        for c in range(CORES):
            source = (l * COLS + col) * CORES + c
            for k in range(CAP):
                index = peer_wanted_s[k, g, source * blk_dev]
                place = (c * CAP + k) * block_len
                peer_out[g, l, place : place + block_len] = cur[half, (l * CORES + c) * blk_dev + index]
        across(l, g).start()

    def take_peer(g):
        half = lax.rem(g, 2)

        def body(i):
            l = level - i
            across(l, g).wait_recv()
            for k in range(picks):
                cur[half, slots_col + l * picks + k] = peer_in[g, l, k * block_len : (k + 1) * block_len]

        loop(level + 1, body)

    factor = math.log2(math.e) * head_width ** (-0.5)
    part = min(rows, 256)
    parts = rows // part
    across_lanes = (((1,), (1,)), ((), ()))

    def score_tile(t, first_group, groups_end):
        tile_number = rank * blk_dev + t
        seen = lax.broadcasted_iota(jnp.int32, (1, nblk), 1) <= tile_number

        def body(g):
            first = pl.multiple_of(g * blk_dev, blk_dev)
            summary = summaries_wide[:, pl.ds(first, blk_dev)].reshape(nblk, head_width).astype(bf16)
            logits = lax.dot_general(queries[g, t], summary, across_lanes, preferred_element_type=f32)
            logits = jnp.where(seen, logits, -jnp.inf)
            top = jnp.max(logits, axis=-1, keepdims=True)
            weights = jnp.exp2((logits - top) * factor)
            totals = jnp.sum(weights, axis=-1, keepdims=True)
            pooled = jnp.sum(weights / totals, axis=0, keepdims=True)
            pooled_ref[pl.ds(t * groups + g, 1), :] = pooled

        loop(groups_end, body, first_group)

    def attend(g, t):
        half = lax.rem(g, 2)
        tile_number = rank * blk_dev + t
        for place in range(TOPN):
            here = slice(place * block_len, (place + 1) * block_len)
            number_here = pick_ref[t, g, place]
            slot = slot_map_s[g, number_here]
            is_own = (number_here == tile_number).astype(jnp.int32)
            key_part[here, :head_width] = cur[half, slot, :, :head_width]
            key_part[here, head_width:] = mask_bank[is_own]
            value_part[here, :head_width] = cur[half, slot, :, head_width:]

        def score(i):
            here = pl.ds(i * part, part)
            query = jnp.concatenate([queries[g, t, here], token_hot[here]], axis=1)
            scores_part[i % 2] = lax.dot_general(
                query, key_part[...], across_lanes, preferred_element_type=f32
            )

        score(0)
        for i in range(parts):
            if i + 1 < parts:
                score(i + 1)
            scores = scores_part[i % 2]
            top = jnp.max(scores, axis=-1, keepdims=True)
            weights = jnp.exp2((scores - top) * factor).astype(bf16)
            mixed = jnp.dot(weights, value_part[...], preferred_element_type=f32)
            result = mixed[:, :head_width] / mixed[:, head_width:]
            wide_out[t, pl.ds(i * part * groups + g, part, stride=groups)] = result

    relay_at = [0] + [(i - 1) * blk_dev // max(levels - 2, 1) for i in range(1, levels)]
    take_at = [0] + [min(spot + 1, blk_dev) for spot in relay_at[1:]]

    def relays(g, t, i):
        @pl.when((t == relay_at[i]) & (level >= i))
        def _():
            relay(g, level - i)

    def takes(g, t, i):
        @pl.when((t == take_at[i]) & (level >= i))
        def _():
            take(g, level - i)

    def main(g):
        @pl.when((g > 0) & (g + lead - 1 < groups - 1))
        def _():
            send_own(g + lead - 1)

        @pl.when(g == groups - 1)
        def _():
            send_own(g)

        def tile(t):
            for i in range(levels):
                if i > 0 and relay_at[i] < blk_dev:
                    relays(g, t, i)
                if take_at[i] < blk_dev:
                    takes(g, t, i)

            @pl.when(g > 0)
            def _():
                attend(g - 1, t)

        loop(blk_dev, tile)
        for i in range(1, levels):
            if relay_at[i] == blk_dev:
                relays(g, blk_dev, i)
        first_tile, end_tile = g * blk_dev // groups, (g + 1) * blk_dev // groups
        loop(end_tile, lambda t: score_tile(t, 0, groups // 2), first_tile)
        for i in range(1, levels):
            if take_at[i] == blk_dev:
                takes(g, blk_dev, i)
        loop(end_tile, lambda t: score_tile(t, groups // 2, groups), first_tile)
        take_peer(g)

    loop(groups, main)

    def last(t):
        attend(groups - 1, t)

        @pl.when(t > 1)
        def _():
            out_copy(t - 2).wait()

        stage[lax.rem(t, 2)] = wide_out[t].reshape(rows, groups, head_width).astype(bf16)
        out_copy(t).start()

    loop(blk_dev, last)

    wanted_copy.wait_send()
    loop(levels, lambda l: keys_up(l, level).wait_send(), level + 1)

    def drain_keys(l):
        keys_aside(l, core).wait_send()
        keys_across(l, col).wait_send()

    loop(level + 1, drain_keys)

    def drain(g):
        def body(l):
            @pl.when(has_above)
            def _():
                up(l, g).wait_send()

            aside(l, g, core).wait_send()
            across(l, g).wait_send()

        loop(level + 1, body)

    loop(groups, drain)
    for t in range(max(blk_dev - 2, 0), blk_dev):
        out_copy(t).wait()


def local(queries, key_rows, value_rows, compressed, chosen):
    _, tok_rows, heads_local, groups, head_width = queries.shape
    block_len = BLOCK
    shards = lax.axis_size("seq")
    seq_rank = lax.axis_index("seq")
    blk_dev = tok_rows // block_len
    nblk = blk_dev * shards
    levels = shards // (COLS * CORES)
    rows = block_len * heads_local

    pick_rows = chosen[0]
    query_tiles = queries[0].reshape(blk_dev, rows, groups, head_width)
    shape = (levels, groups, blk_dev, heads_local, block_len, head_width)
    wide = 2 * head_width
    served = CORES * CAP * block_len
    part = min(rows, 256)
    dma = pltpu.SemaphoreType.DMA
    smem = pl.BlockSpec(memory_space=pltpu.SMEM)
    vmem = pl.BlockSpec(memory_space=pltpu.VMEM)
    anyspace = pl.BlockSpec(memory_space=pl.ANY)
    slots = levels * CORES * (blk_dev + CAP)
    bf16, f32 = jnp.bfloat16, jnp.float32
    attended, pooled = pl.pallas_call(
        functools.partial(mega, shape),
        in_specs=[smem, vmem, vmem, anyspace, anyspace, anyspace],
        out_specs=[anyspace, vmem],
        out_shape=[
            jax.ShapeDtypeStruct((blk_dev, rows, groups, head_width), bf16),
            jax.ShapeDtypeStruct((blk_dev * groups, nblk), f32),
        ],
        scratch_shapes=[
            pltpu.VMEM((levels, CORES, groups, tok_rows, wide), bf16),
            pltpu.VMEM((groups, levels, served, wide), bf16),
            pltpu.VMEM((groups, levels, served, wide), bf16),
            pltpu.VMEM((2, slots, block_len, wide), bf16),
            pltpu.VMEM((levels, COLS, CORES, groups * blk_dev, head_width), bf16),
            pltpu.VMEM((shards, groups * blk_dev, head_width), f32),
            pltpu.VMEM((groups, blk_dev, rows, head_width), bf16),
            pltpu.VMEM((blk_dev, rows * groups, head_width), f32),
            pltpu.VMEM((2, rows, groups, head_width), bf16),
            pltpu.VMEM((2, tok_rows, groups, head_width), bf16),
            pltpu.VMEM((TOPN * block_len, wide), bf16),
            pltpu.VMEM((TOPN * block_len, wide), bf16),
            pltpu.VMEM((2, part, TOPN * block_len), f32),
            pltpu.VMEM((rows, head_width), bf16),
            pltpu.VMEM((2, block_len, head_width), bf16),
            pltpu.VMEM((groups, nblk), jnp.int32),
            pltpu.SMEM((groups, nblk), jnp.int32),
            pltpu.VMEM((CAP, groups, nblk), jnp.int32),
            pltpu.VMEM((CAP, groups, nblk), jnp.int32),
            pltpu.SMEM((CAP, groups, nblk), jnp.int32),
        ]
        + [dma((levels, groups))] * 6
        + [dma((3, levels))] * 2
        + [dma((2,)), dma((6,))],
        compiler_params=pltpu.CompilerParams(
            collective_id=0, has_side_effects=True, vmem_limit_bytes=67043328
        ),
    )(pick_rows, pick_rows, compressed[0], key_rows[0], value_rows[0], query_tiles)
    pooled = pooled.reshape(1, blk_dev, groups, nblk)
    shared = lax.psum_scatter(pooled, "head", scatter_dimension=2, tiled=True)
    tile_ids = seq_rank * blk_dev + jnp.arange(blk_dev, dtype=jnp.int32)
    factor = (tile_ids + 1).astype(jnp.float32) / (block_len * HPG)
    block_scores = shared * factor[None, :, None, None]
    attended = attended.reshape(1, tok_rows, heads_local, groups, head_width)
    return (block_scores, attended)


def solution(mesh):
    placed = (
        P("batch", "seq", "head", None, None),
        P("batch", "seq", None, None),
        P("batch", "seq", None, None),
        P("batch", "seq", None, None),
        P("batch", "seq", None, None),
    )
    return jax.shard_map(
        local,
        mesh=mesh,
        in_specs=placed,
        out_specs=(P("batch", "seq", "head", None), P("batch", "seq", "head", None, None)),
        check_vma=False,
    )
```

```python
import functools
import math

import jax
import jax.numpy as jnp
from jax import lax
from jax.experimental import pallas as pl
from jax.experimental.pallas import tpu as pltpu
from jax.sharding import PartitionSpec as P

HPG = 8
BLOCK = 64
TOPN = 16
CAP = 2
COLS = 2
CORES = 2
MESH = pl.DeviceIdType.MESH


def prepare(shape, token_hot, mask_bank, value_part):
    _, _, _, heads_local, block_len, head_width = shape
    rows = block_len * heads_local
    row_token = lax.broadcasted_iota(jnp.int32, (rows, head_width), 0) // heads_local
    row_lane = lax.broadcasted_iota(jnp.int32, (rows, head_width), 1)
    token_hot[...] = jnp.where(row_token == row_lane, 1.0, 0.0).astype(jnp.bfloat16)
    key_place = lax.broadcasted_iota(jnp.int32, (block_len, head_width), 0)
    key_lane = lax.broadcasted_iota(jnp.int32, (block_len, head_width), 1)
    mask_bank[0] = jnp.zeros((block_len, head_width), jnp.bfloat16)
    mask_bank[1] = jnp.where(key_place > key_lane, -1e30, 0.0).astype(jnp.bfloat16)
    value_part[:, head_width:] = jnp.ones((TOPN * block_len, head_width), jnp.bfloat16)


def attend_unit(shape, pool, number_at, slot_at, tile_number, query_at, store, work):
    _, _, _, heads_local, block_len, head_width = shape
    key_part, value_part, scores_part, token_hot, mask_bank = work
    rows = block_len * heads_local
    part = min(rows, 256)
    parts = rows // part
    factor = math.log2(math.e) * head_width ** (-0.5)
    for place in range(TOPN):
        here = slice(place * block_len, (place + 1) * block_len)
        number = number_at(place)
        slot = slot_at(number)
        is_own = (number == tile_number).astype(jnp.int32)
        key_part[here, :head_width] = pool[slot, :, :head_width]
        key_part[here, head_width:] = mask_bank[is_own]
        value_part[here, :head_width] = pool[slot, :, head_width:]

    def score(i):
        here = pl.ds(i * part, part)
        query = jnp.concatenate([query_at(here), token_hot[here]], axis=1)
        scores_part[i % 2] = lax.dot_general(
            query, key_part[...], (((1,), (1,)), ((), ())), preferred_element_type=jnp.float32
        )

    score(0)
    for i in range(parts):
        if i + 1 < parts:
            score(i + 1)
        scores = scores_part[i % 2]
        top = jnp.max(scores, axis=-1, keepdims=True)
        weights = jnp.exp2((scores - top) * factor).astype(jnp.bfloat16)
        mixed = jnp.dot(weights, value_part[...], preferred_element_type=jnp.float32)
        store(i * part, part, mixed[:, :head_width] / mixed[:, head_width:])


def finish(
    shape,
    pick_ref,
    slot_ref,
    partial_ref,
    query_ref,
    pool_ref,
    pooled_ref,
    out_ref,
    block_scores_ref,
    wide,
    key_part,
    value_part,
    scores_part,
    token_hot,
    mask_bank,
):
    _, groups, blk_dev, heads_local, block_len, head_width = shape
    rows = block_len * heads_local
    rank = lax.axis_index("seq")
    t = pl.program_id(0)
    last = groups - 1

    @pl.when(t == 0)
    def _():
        prepare(shape, token_hot, mask_bank, value_part)
        lines = pooled_ref.shape[0]
        line_tile = lax.broadcasted_iota(jnp.int32, (lines, 1), 0) // (lines // blk_dev)
        scale = (rank * blk_dev + line_tile + 1).astype(jnp.float32) / (block_len * HPG)
        block_scores_ref[...] = pooled_ref[...] * scale

    wide[...] = partial_ref[0].astype(jnp.float32).reshape(rows * groups, head_width)

    def store(start, count, result):
        wide[pl.ds(start * groups + last, count, stride=groups)] = result

    attend_unit(
        shape,
        pool_ref,
        lambda place: pick_ref[t, last, place],
        lambda number: slot_ref[last, number],
        rank * blk_dev + t,
        lambda here: query_ref[0, here],
        store,
        (key_part, value_part, scores_part, token_hot, mask_bank),
    )
    out_ref[0] = wide[...].reshape(rows, groups, head_width).astype(jnp.bfloat16)


def mega(
    shape,
    pick_ref,
    chosen_ref,
    summary_ref,
    key_ref,
    value_ref,
    query_ref,
    out_ref,
    pooled_ref,
    pool_out,
    query_out,
    slot_out,
    column,
    peer_out,
    peer_in,
    cur,
    summaries,
    summaries_wide,
    queries,
    wide_out,
    stage,
    rows_stage,
    key_part,
    value_part,
    scores_part,
    token_hot,
    mask_bank,
    slot_map,
    slot_map_s,
    wanted,
    peer_wanted,
    peer_wanted_s,
    up_send,
    up_recv,
    sib_send,
    sib_recv,
    peer_send,
    peer_recv,
    key_send,
    key_recv,
    stage_sem,
    pool_sem,
    misc_sem,
):
    levels, groups, blk_dev, heads_local, block_len, head_width = shape
    rows = block_len * heads_local
    per_level = COLS * CORES
    slots_col = levels * CORES * blk_dev
    picks = CORES * CAP
    f32, bf16 = jnp.float32, jnp.bfloat16

    rank = lax.axis_index("seq")
    core = lax.rem(rank, CORES)
    col = lax.rem(rank // CORES, COLS)
    level = rank // per_level
    sibling = rank + 1 - 2 * core
    peer = rank + CORES * (1 - 2 * col)
    above = rank + per_level
    has_above = level < levels - 1

    def loop(n, body, start=0):
        def step(i, carry):
            body(i)
            return carry

        lax.fori_loop(start, n, step, 0)

    barrier = pltpu.get_barrier_semaphore()
    for other in (sibling, peer):
        pl.semaphore_signal(barrier, inc=1, device_id={"seq": other}, device_id_type=MESH)
    for step in range(1, levels):
        other = lax.rem(rank + step * per_level, levels * per_level)
        pl.semaphore_signal(barrier, inc=1, device_id={"seq": other}, device_id_type=MESH)

    def query_copy(t):
        half = lax.rem(t, 2)
        return pltpu.make_async_copy(query_ref.at[t], stage.at[half], stage_sem.at[half])

    def out_copy(t):
        half = lax.rem(t, 2)
        return pltpu.make_async_copy(stage.at[half], out_ref.at[t], stage_sem.at[half])

    def remote(src, dst, send, recv, device):
        return pltpu.make_async_remote_copy(
            src, dst, send, recv, device_id={"seq": device}, device_id_type=MESH
        )

    def up(l, g):
        part = column.at[l, core, g]
        return remote(part, part, up_send.at[l, g], up_recv.at[l, g], above)

    def aside(l, g, owner):
        part = column.at[l, owner, g]
        return remote(part, part, sib_send.at[l, g], sib_recv.at[l, g], sibling)

    def across(l, g):
        return remote(peer_out.at[g, l], peer_in.at[g, l], peer_send.at[l, g], peer_recv.at[l, g], peer)

    def keys_up(l, source):
        part = summaries.at[source, col, core]
        return remote(part, part, key_send.at[0, l], key_recv.at[0, source], rank + (l - level) * per_level)

    def keys_aside(l, owner):
        part = summaries.at[l, col, owner]
        return remote(part, part, key_send.at[1, l], key_recv.at[1, l], sibling)

    def keys_across(l, owner):
        part = summaries.at[l, owner]
        return remote(part, part, key_send.at[2, l], key_recv.at[2, l], peer)

    wanted_copy = remote(wanted, peer_wanted, misc_sem.at[0], misc_sem.at[1], peer)
    slots_copy = pltpu.make_async_copy(slot_map, slot_map_s, misc_sem.at[2])
    loads = [
        pltpu.make_async_copy(key_ref, rows_stage.at[0], misc_sem.at[4]),
        pltpu.make_async_copy(value_ref, rows_stage.at[1], misc_sem.at[5]),
    ]
    for load in loads:
        load.start()
    query_copy(0).start()

    nblk = levels * per_level * blk_dev
    number = lax.broadcasted_iota(jnp.int32, (groups, nblk), 1)
    named = jnp.zeros((groups, nblk), jnp.int32)
    for t in range(blk_dev):
        picks_here = chosen_ref[t]
        for place in range(TOPN):
            named = jnp.where(picks_here[:, place : place + 1] == number, 1, named)
    inside = lax.rem(number, blk_dev)
    order = named
    step = 1
    while step < blk_dev:
        order = order + jnp.where(inside >= step, pltpu.roll(order, step, 1), 0)
        step *= 2
    order = order - named
    for k in range(CAP):
        found = jnp.where((named == 1) & (order == k), inside, 0)
        step = 1
        while step < blk_dev:
            found = found + pltpu.roll(found, nblk - step, 1)
            step *= 2
        wanted[k] = found
    device = number // blk_dev
    pair = device // per_level * CORES + lax.rem(device, CORES)
    in_column = lax.rem(device // CORES, COLS) == col
    slot_map[...] = jnp.where(in_column, pair * blk_dev + inside, slots_col + pair * CAP + order)

    own_summary = jnp.swapaxes(summary_ref[...].astype(f32), 0, 1)
    own_summary = own_summary.reshape(groups * blk_dev, head_width).astype(bf16)
    summaries[level, col, core] = own_summary
    prepare(shape, token_hot, mask_bank, value_part)
    summaries_wide[...] = jnp.zeros_like(summaries_wide)
    for kind in range(2):
        loads[kind].wait()

        def split(r, kind=kind):
            here = pl.ds(pl.multiple_of(r * block_len, block_len), block_len)
            apart = jnp.swapaxes(rows_stage[kind, here].astype(f32), 0, 1).astype(bf16)
            for g in range(groups):
                column[level, core, g, here, kind * head_width : (kind + 1) * head_width] = apart[g]

        loop(blk_dev, split)
    slots_copy.start()
    pl.semaphore_wait(barrier, levels + 1)

    loop(levels, lambda l: keys_up(l, level).start(), level + 1)
    keys_aside(level, core).start()
    wanted_copy.start()

    def send_own(g):
        @pl.when(has_above)
        def _():
            up(level, g).start()

    lead = jnp.where(level == 0, groups, jnp.where(level == levels - 2, min(3, groups), 1))
    loop(lead, send_own)
    loop(groups, lambda g: aside(level, g, core).start())

    def spread(t):
        query_copy(t).wait()

        @pl.when(t + 1 < blk_dev)
        def _():
            query_copy(t + 1).start()

        half = lax.rem(t, 2)
        wide_out[t] = stage[half].astype(f32).reshape(rows * groups, head_width)
        for g in range(groups):
            queries[g, t] = wide_out[t, pl.ds(g, rows, stride=groups)].astype(bf16)

    loop(blk_dev, spread)
    handed_on = [
        pltpu.make_async_copy(queries.at[groups - 1], query_out, misc_sem.at[6]),
        pltpu.make_async_copy(slot_map, slot_out, misc_sem.at[7]),
    ]
    for copy in handed_on:
        copy.start()

    def relay_keys(l):
        keys_up(l, l).wait_recv()
        keys_aside(l, core).start()

    def pair_keys(l):
        keys_aside(l, 1 - core).wait_recv()
        keys_across(l, col).start()

    def widen_keys(l):
        keys_across(l, 1 - col).wait_recv()
        for x in range(COLS):
            for c in range(CORES):
                summaries_wide[(l * COLS + x) * CORES + c] = summaries[l, x, c].astype(f32)

    loop(level, relay_keys)
    loop(level + 1, pair_keys)
    wanted_copy.wait_recv()
    local_wanted = pltpu.make_async_copy(peer_wanted, peer_wanted_s, misc_sem.at[3])
    local_wanted.start()
    local_wanted.wait()
    slots_copy.wait()
    loop(level + 1, widen_keys)

    def relay(g, l):
        up(l, g).wait_recv()

        @pl.when(has_above)
        def _():
            up(l, g).start()

        aside(l, g, core).start()

    def take(g, l):
        half = lax.rem(g, 2)
        aside(l, g, 1 - core).wait_recv()
        for c in range(CORES):
            first = (l * CORES + c) * blk_dev
            for b in range(blk_dev):
                cur[half, first + b] = column[l, c, g, b * block_len : (b + 1) * block_len]
        for c in range(CORES):
            source = (l * COLS + col) * CORES + c
            for k in range(CAP):
                index = peer_wanted_s[k, g, source * blk_dev]
                place = (c * CAP + k) * block_len
                peer_out[g, l, place : place + block_len] = cur[half, (l * CORES + c) * blk_dev + index]
        across(l, g).start()

        @pl.when(g == groups - 1)
        def _():
            pool_copy(0, l).start()

    def take_peer(g):
        half = lax.rem(g, 2)

        def body(i):
            l = level - i
            across(l, g).wait_recv()
            for k in range(picks):
                cur[half, slots_col + l * picks + k] = peer_in[g, l, k * block_len : (k + 1) * block_len]

            @pl.when(g == groups - 1)
            def _():
                pool_copy(1, l).start()

        loop(level + 1, body)

    factor = math.log2(math.e) * head_width ** (-0.5)
    across_lanes = (((1,), (1,)), ((), ()))

    def score_tile(t, first_group, groups_end):
        tile_number = rank * blk_dev + t
        seen = lax.broadcasted_iota(jnp.int32, (1, nblk), 1) <= tile_number

        def body(g):
            first = pl.multiple_of(g * blk_dev, blk_dev)
            summary = summaries_wide[:, pl.ds(first, blk_dev)].reshape(nblk, head_width).astype(bf16)
            logits = lax.dot_general(queries[g, t], summary, across_lanes, preferred_element_type=f32)
            logits = jnp.where(seen, logits, -jnp.inf)
            top = jnp.max(logits, axis=-1, keepdims=True)
            weights = jnp.exp2((logits - top) * factor)
            totals = jnp.sum(weights, axis=-1, keepdims=True)
            pooled = jnp.sum(weights / totals, axis=0, keepdims=True)
            pooled_ref[pl.ds(t * groups + g, 1), :] = pooled

        loop(groups_end, body, first_group)

    def attend(g, t):
        half = lax.rem(g, 2)

        def store(start, count, result):
            wide_out[t, pl.ds(start * groups + g, count, stride=groups)] = result

        attend_unit(
            shape,
            cur.at[half],
            lambda place: pick_ref[t, g, place],
            lambda number: slot_map_s[g, number],
            rank * blk_dev + t,
            lambda here: queries[g, t, here],
            store,
            (key_part, value_part, scores_part, token_hot, mask_bank),
        )

    def put_out(t):
        @pl.when(t > 1)
        def _():
            out_copy(t - 2).wait()

        stage[lax.rem(t, 2)] = wide_out[t].reshape(rows, groups, head_width).astype(bf16)
        out_copy(t).start()

    def pool_copy(kind, l):
        count = (CORES * blk_dev, picks)[kind]
        here = pl.ds(kind * slots_col + l * count, count)
        return pltpu.make_async_copy(cur.at[(groups - 1) % 2, here], pool_out.at[here], pool_sem.at[kind, l])

    relay_at = [0] + [(i - 1) * (blk_dev - 2) // max(levels - 2, 1) for i in range(1, levels)]
    take_at = [0] + [min(spot + 1, blk_dev) for spot in relay_at[1:]]

    def relays(g, t, i):
        @pl.when((t == relay_at[i]) & (level >= i))
        def _():
            relay(g, level - i)

        @pl.when((t == relay_at[i]) & (level == i) & (g + 1 >= lead) & (g + 1 < groups))
        def _():
            send_own(g + 1)

    def takes(g, t, i):
        @pl.when((t == take_at[i]) & (level >= i))
        def _():
            take(g, level - i)

    def main(g):
        def tile(t):
            for i in range(levels):
                if i > 0 and relay_at[i] < blk_dev:
                    relays(g, t, i)
                if take_at[i] < blk_dev:
                    takes(g, t, i)

            @pl.when(g > 0)
            def _():
                attend(g - 1, t)

            @pl.when(g == groups - 1)
            def _():
                put_out(t)

        loop(blk_dev, tile)
        for i in range(1, levels):
            if relay_at[i] == blk_dev:
                relays(g, blk_dev, i)
        first_tile, end_tile = g * blk_dev // groups, (g + 1) * blk_dev // groups
        loop(end_tile, lambda t: score_tile(t, 0, groups // 2), first_tile)
        for i in range(1, levels):
            if take_at[i] == blk_dev:
                takes(g, blk_dev, i)
        loop(end_tile, lambda t: score_tile(t, groups // 2, groups), first_tile)
        take_peer(g)

    loop(groups, main)

    wanted_copy.wait_send()
    loop(levels, lambda l: keys_up(l, level).wait_send(), level + 1)

    def drain_keys(l):
        pool_copy(0, l).wait()
        pool_copy(1, l).wait()
        keys_aside(l, core).wait_send()
        keys_across(l, col).wait_send()

    loop(level + 1, drain_keys)

    def drain(g):
        def body(l):
            @pl.when(has_above)
            def _():
                up(l, g).wait_send()

            aside(l, g, core).wait_send()
            across(l, g).wait_send()

        loop(level + 1, body)

    loop(groups, drain)
    for t in range(max(blk_dev - 2, 0), blk_dev):
        out_copy(t).wait()
    for copy in handed_on:
        copy.wait()


def local(queries, key_rows, value_rows, compressed, chosen):
    _, tok_rows, heads_local, groups, head_width = queries.shape
    block_len = BLOCK
    shards = lax.axis_size("seq")
    blk_dev = tok_rows // block_len
    nblk = blk_dev * shards
    levels = shards // (COLS * CORES)
    rows = block_len * heads_local

    pick_rows = chosen[0]
    query_tiles = queries[0].reshape(blk_dev, rows, groups, head_width)
    shape = (levels, groups, blk_dev, heads_local, block_len, head_width)
    wide = 2 * head_width
    served = CORES * CAP * block_len
    part = min(rows, 256)
    dma = pltpu.SemaphoreType.DMA
    smem = pl.BlockSpec(memory_space=pltpu.SMEM)
    vmem = pl.BlockSpec(memory_space=pltpu.VMEM)
    anyspace = pl.BlockSpec(memory_space=pl.ANY)
    slots = levels * CORES * (blk_dev + CAP)
    bf16, f32 = jnp.bfloat16, jnp.float32
    partial, pooled, pool, last_queries, slot_map = pl.pallas_call(
        functools.partial(mega, shape),
        in_specs=[smem, vmem, vmem, anyspace, anyspace, anyspace],
        out_specs=[anyspace, vmem, anyspace, anyspace, anyspace],
        out_shape=[
            jax.ShapeDtypeStruct((blk_dev, rows, groups, head_width), bf16),
            jax.ShapeDtypeStruct((blk_dev * groups, nblk), f32),
            jax.ShapeDtypeStruct((slots, block_len, wide), bf16),
            jax.ShapeDtypeStruct((blk_dev, rows, head_width), bf16),
            jax.ShapeDtypeStruct((groups, nblk), jnp.int32),
        ],
        scratch_shapes=[
            pltpu.VMEM((levels, CORES, groups, tok_rows, wide), bf16),
            pltpu.VMEM((groups, levels, served, wide), bf16),
            pltpu.VMEM((groups, levels, served, wide), bf16),
            pltpu.VMEM((2, slots, block_len, wide), bf16),
            pltpu.VMEM((levels, COLS, CORES, groups * blk_dev, head_width), bf16),
            pltpu.VMEM((shards, groups * blk_dev, head_width), f32),
            pltpu.VMEM((groups, blk_dev, rows, head_width), bf16),
            pltpu.VMEM((blk_dev, rows * groups, head_width), f32),
            pltpu.VMEM((2, rows, groups, head_width), bf16),
            pltpu.VMEM((2, tok_rows, groups, head_width), bf16),
            pltpu.VMEM((TOPN * block_len, wide), bf16),
            pltpu.VMEM((TOPN * block_len, wide), bf16),
            pltpu.VMEM((2, part, TOPN * block_len), f32),
            pltpu.VMEM((rows, head_width), bf16),
            pltpu.VMEM((2, block_len, head_width), bf16),
            pltpu.VMEM((groups, nblk), jnp.int32),
            pltpu.SMEM((groups, nblk), jnp.int32),
            pltpu.VMEM((CAP, groups, nblk), jnp.int32),
            pltpu.VMEM((CAP, groups, nblk), jnp.int32),
            pltpu.SMEM((CAP, groups, nblk), jnp.int32),
        ]
        + [dma((levels, groups))] * 6
        + [dma((3, levels))] * 2
        + [dma((2,)), dma((2, levels)), dma((8,))],
        compiler_params=pltpu.CompilerParams(
            collective_id=0, has_side_effects=True, vmem_limit_bytes=67043328
        ),
    )(pick_rows, pick_rows, compressed[0], key_rows[0], value_rows[0], query_tiles)
    pooled = pooled.reshape(1, blk_dev, groups, nblk)
    shared = lax.psum_scatter(pooled, "head", scatter_dimension=2, tiled=True)
    groups_out = shared.shape[2]
    whole = pl.BlockSpec((slots, block_len, wide), lambda t: (0, 0, 0))
    lines = pl.BlockSpec((blk_dev * groups_out, nblk), lambda t: (0, 0))
    tile = pl.BlockSpec((1, rows, groups, head_width), lambda t: (t, 0, 0, 0))
    attended, block_scores = pl.pallas_call(
        functools.partial(finish, shape),
        grid=(blk_dev,),
        in_specs=[smem, smem, tile, pl.BlockSpec((1, rows, head_width), lambda t: (t, 0, 0)), whole, lines],
        out_specs=[tile, lines],
        out_shape=[
            jax.ShapeDtypeStruct((blk_dev, rows, groups, head_width), bf16),
            jax.ShapeDtypeStruct((blk_dev * groups_out, nblk), f32),
        ],
        scratch_shapes=[
            pltpu.VMEM((rows * groups, head_width), f32),
            pltpu.VMEM((TOPN * block_len, wide), bf16),
            pltpu.VMEM((TOPN * block_len, wide), bf16),
            pltpu.VMEM((2, part, TOPN * block_len), f32),
            pltpu.VMEM((rows, head_width), bf16),
            pltpu.VMEM((2, block_len, head_width), bf16),
        ],
        compiler_params=pltpu.CompilerParams(
            dimension_semantics=("arbitrary",), vmem_limit_bytes=67043328
        ),
    )(pick_rows, slot_map, partial, last_queries, pool, shared.reshape(blk_dev * groups_out, nblk))
    block_scores = block_scores.reshape(1, blk_dev, groups_out, nblk)
    attended = attended.reshape(1, tok_rows, heads_local, groups, head_width)
    return (block_scores, attended)


def solution(mesh):
    placed = (
        P("batch", "seq", "head", None, None),
        P("batch", "seq", None, None),
        P("batch", "seq", None, None),
        P("batch", "seq", None, None),
        P("batch", "seq", None, None),
    )
    return jax.shard_map(
        local,
        mesh=mesh,
        in_specs=placed,
        out_specs=(P("batch", "seq", "head", None), P("batch", "seq", "head", None, None)),
        check_vma=False,
    )
```

```python
import functools
import math

import jax
import jax.numpy as jnp
from jax import lax
from jax.experimental import pallas as pl
from jax.experimental.pallas import tpu as pltpu
from jax.sharding import PartitionSpec as P

HPG = 8
BLOCK = 64
TOPN = 16
CAP = 2
COLS = 2
CORES = 2
MESH = pl.DeviceIdType.MESH


def prepare(shape, token_hot, mask_bank, value_parts):
    _, _, _, heads_local, block_len, head_width = shape
    rows = block_len * heads_local
    row_token = lax.broadcasted_iota(jnp.int32, (rows, head_width), 0) // heads_local
    row_lane = lax.broadcasted_iota(jnp.int32, (rows, head_width), 1)
    token_hot[...] = jnp.where(row_token == row_lane, 1.0, 0.0).astype(jnp.bfloat16)
    key_place = lax.broadcasted_iota(jnp.int32, (block_len, head_width), 0)
    key_lane = lax.broadcasted_iota(jnp.int32, (block_len, head_width), 1)
    mask_bank[0] = jnp.zeros((block_len, head_width), jnp.bfloat16)
    mask_bank[1] = jnp.where(key_place > key_lane, -1e30, 0.0).astype(jnp.bfloat16)
    lanes = value_parts.shape[2] - head_width
    for i in range(value_parts.shape[0]):
        value_parts[i, :, head_width:] = jnp.ones((TOPN * block_len, lanes), jnp.bfloat16)


def attend_units(shape, pool, units, work):
    _, _, _, heads_local, block_len, head_width = shape
    key_parts, value_parts, scores_parts, token_hot, mask_bank = work
    rows = block_len * heads_local
    part = min(rows, 256)
    parts = rows // part
    factor = math.log2(math.e) * head_width ** (-0.5)

    def gather(u):
        number_at, slot_at, tile_number, _, _ = units[u]
        for place in range(TOPN):
            here = slice(place * block_len, (place + 1) * block_len)
            number = number_at(place)
            slot = slot_at(number)
            is_own = (number == tile_number).astype(jnp.int32)
            key_parts[u, here, :head_width] = pool[slot, :, :head_width]
            key_parts[u, here, head_width:] = mask_bank[is_own]
            value_parts[u, here, :head_width] = pool[slot, :, head_width:]

    def score(u, i):
        here = pl.ds(i * part, part)
        query = jnp.concatenate([units[u][3](here), token_hot[here]], axis=1)
        scores_parts[u, i % 2] = lax.dot_general(
            query, key_parts[u], (((1,), (1,)), ((), ())), preferred_element_type=jnp.float32
        )

    def mix(u, i):
        scores = scores_parts[u, i % 2]
        top = jnp.max(scores, axis=-1, keepdims=True)
        weights = jnp.exp2((scores - top) * factor).astype(jnp.bfloat16)
        mixed = jnp.dot(weights, value_parts[u], preferred_element_type=jnp.float32)
        units[u][4](i * part, part, mixed[:, :head_width] / mixed[:, head_width:])

    steps = [(u, i) for u in range(len(units)) for i in range(parts)]
    gather(0)
    score(0, 0)
    for n, (u, i) in enumerate(steps):
        if n + 1 < len(steps):
            ahead = steps[n + 1]
            if i == 0 and u + 1 < len(units):
                gather(u + 1)
            score(*ahead)
        mix(u, i)


def finish(
    shape,
    pick_ref,
    slot_ref,
    partial_ref,
    query_ref,
    pool_ref,
    pooled_ref,
    out_ref,
    block_scores_ref,
    wide,
    key_parts,
    value_parts,
    scores_parts,
    token_hot,
    mask_bank,
):
    _, groups, blk_dev, heads_local, block_len, head_width = shape
    rows = block_len * heads_local
    rank = lax.axis_index("seq")
    step = pl.program_id(0)
    last = groups - 1
    width = wide.shape[0]

    @pl.when(step == 0)
    def _():
        prepare(shape, token_hot, mask_bank, value_parts)
        lines = pooled_ref.shape[0]
        line_tile = lax.broadcasted_iota(jnp.int32, (lines, 1), 0) // (lines // blk_dev)
        scale = (rank * blk_dev + line_tile + 1).astype(jnp.float32) / (block_len * HPG)
        block_scores_ref[...] = pooled_ref[...] * scale

    def unit(u):
        t = step * width + u

        def store(start, count, result):
            wide[u, pl.ds(start * groups + last, count, stride=groups)] = result

        return (
            lambda place: pick_ref[t, last, place],
            lambda number: slot_ref[last, number],
            rank * blk_dev + t,
            lambda here: query_ref[u, here],
            store,
        )

    for u in range(width):
        wide[u] = partial_ref[u].astype(jnp.float32).reshape(rows * groups, head_width)
    work = (key_parts, value_parts, scores_parts, token_hot, mask_bank)
    attend_units(shape, pool_ref, [unit(u) for u in range(width)], work)
    for u in range(width):
        out_ref[u] = wide[u].reshape(rows, groups, head_width).astype(jnp.bfloat16)


def mega(
    shape,
    pick_ref,
    chosen_ref,
    summary_ref,
    key_ref,
    value_ref,
    query_ref,
    out_ref,
    pooled_ref,
    pool_out,
    query_out,
    slot_out,
    column,
    peer_out,
    peer_in,
    cur,
    summaries,
    summaries_wide,
    queries,
    wide_out,
    stage,
    key_parts,
    value_parts,
    scores_parts,
    token_hot,
    mask_bank,
    slot_map,
    slot_map_s,
    wanted,
    peer_wanted,
    peer_wanted_s,
    up_send,
    up_recv,
    sib_send,
    sib_recv,
    peer_send,
    peer_recv,
    key_send,
    key_recv,
    stage_sem,
    pool_sem,
    misc_sem,
):
    levels, groups, blk_dev, heads_local, block_len, head_width = shape
    rows = block_len * heads_local
    tokens = blk_dev * block_len
    per_level = COLS * CORES
    nblk = levels * per_level * blk_dev
    slots_col = levels * CORES * blk_dev
    picks = CORES * CAP
    f32, bf16 = jnp.float32, jnp.bfloat16

    rank = lax.axis_index("seq")
    core = lax.rem(rank, CORES)
    col = lax.rem(rank // CORES, COLS)
    level = rank // per_level
    sibling = rank + 1 - 2 * core
    peer = rank + CORES * (1 - 2 * col)
    above = rank + per_level
    has_above = level < levels - 1

    def loop(n, body, start=0):
        def step(i, carry):
            body(i)
            return carry

        lax.fori_loop(start, n, step, 0)

    barrier = pltpu.get_barrier_semaphore()
    for other in (sibling, peer):
        pl.semaphore_signal(barrier, inc=1, device_id={"seq": other}, device_id_type=MESH)
    for step in range(1, levels):
        other = lax.rem(rank + step * per_level, levels * per_level)
        pl.semaphore_signal(barrier, inc=1, device_id={"seq": other}, device_id_type=MESH)

    def query_copy(t):
        half = lax.rem(t, 2)
        return pltpu.make_async_copy(query_ref.at[t], stage.at[half], stage_sem.at[half])

    def out_copy(t):
        half = lax.rem(t, 2)
        return pltpu.make_async_copy(stage.at[half], out_ref.at[t], stage_sem.at[half])

    def remote(src, dst, send, recv, device):
        return pltpu.make_async_remote_copy(
            src, dst, send, recv, device_id={"seq": device}, device_id_type=MESH
        )

    def up(l, g):
        part = column.at[l, core, g]
        return remote(part, part, up_send.at[l, g], up_recv.at[l, g], above)

    def aside(l, g, owner):
        part = column.at[l, owner, g]
        return remote(part, part, sib_send.at[l, g], sib_recv.at[l, g], sibling)

    def across(l, g):
        return remote(peer_out.at[g, l], peer_in.at[g, l], peer_send.at[l, g], peer_recv.at[l, g], peer)

    def keys_up(l, source):
        part = summaries.at[source, col, core]
        return remote(part, part, key_send.at[0, l], key_recv.at[0, source], rank + (l - level) * per_level)

    def keys_aside(l, owner):
        part = summaries.at[l, col, owner]
        return remote(part, part, key_send.at[1, l], key_recv.at[1, l], sibling)

    def keys_across(l, owner):
        part = summaries.at[l, owner]
        return remote(part, part, key_send.at[2, l], key_recv.at[2, l], peer)

    wanted_copy = remote(wanted, peer_wanted, misc_sem.at[0], misc_sem.at[1], peer)
    slots_copy = pltpu.make_async_copy(slot_map, slot_map_s, misc_sem.at[2])
    def load(slab, kind, ref):
        return pltpu.make_async_copy(
            ref.at[slab * rows : (slab + 1) * rows], stage.at[kind], misc_sem.at[4 + kind]
        )

    load(0, 0, key_ref).start()
    load(0, 1, value_ref).start()

    own_summary = jnp.swapaxes(summary_ref[...].astype(f32), 0, 1)
    own_summary = own_summary.reshape(groups * blk_dev, head_width).astype(bf16)
    summaries[level, col, core] = own_summary
    for slab in range(tokens // rows):
        for kind, ref in enumerate((key_ref, value_ref)):
            load(slab, kind, ref).wait()

            def split(r, slab=slab, kind=kind):
                source = pl.ds(pl.multiple_of(r * block_len, block_len), block_len)
                place = pl.multiple_of(slab * rows + r * block_len, block_len)
                apart = jnp.swapaxes(stage[kind, source].astype(f32), 0, 1).astype(bf16)
                lanes = slice(kind * head_width, (kind + 1) * head_width)
                for g in range(groups):
                    column[level, core, g, pl.ds(place, block_len), lanes] = apart[g]

            loop(heads_local, split)
            if (slab + 1) * rows < tokens:
                load(slab + 1, kind, ref).start()
    query_copy(0).start()
    pl.semaphore_wait(barrier, levels + 1)

    loop(levels, lambda l: keys_up(l, level).start(), level + 1)
    keys_aside(level, core).start()

    def send_own(g):
        @pl.when(has_above)
        def _():
            up(level, g).start()

    lead = jnp.where(level == 0, groups, jnp.where(level == levels - 2, min(3, groups), 1))
    loop(lead, send_own)
    loop(groups, lambda g: aside(level, g, core).start())

    number = lax.broadcasted_iota(jnp.int32, (groups, nblk), 1)
    named = jnp.zeros((groups, nblk), jnp.int32)
    for t in range(blk_dev):
        picks_here = chosen_ref[t]
        for place in range(TOPN):
            named = jnp.where(picks_here[:, place : place + 1] == number, 1, named)
    inside = lax.rem(number, blk_dev)
    order = named
    step = 1
    while step < blk_dev:
        order = order + jnp.where(inside >= step, pltpu.roll(order, step, 1), 0)
        step *= 2
    order = order - named
    for k in range(CAP):
        found = jnp.where((named == 1) & (order == k), inside, 0)
        step = 1
        while step < blk_dev:
            found = found + pltpu.roll(found, nblk - step, 1)
            step *= 2
        wanted[k] = found
    device = number // blk_dev
    pair = device // per_level * CORES + lax.rem(device, CORES)
    in_column = lax.rem(device // CORES, COLS) == col
    slot_map[...] = jnp.where(in_column, pair * blk_dev + inside, slots_col + pair * CAP + order)

    prepare(shape, token_hot, mask_bank, value_parts)
    summaries_wide[...] = jnp.zeros_like(summaries_wide)
    wanted_copy.start()
    slots_copy.start()

    def relay(g, l):
        up(l, g).wait_recv()

        @pl.when(has_above)
        def _():
            up(l, g).start()

        aside(l, g, core).start()

    def early(g):
        relay(g, level - 1)

        @pl.when((level == 1) & (g + 1 >= lead) & (g + 1 < groups))
        def _():
            send_own(g + 1)

    def spread(t):
        query_copy(t).wait()

        @pl.when(t + 1 < blk_dev)
        def _():
            query_copy(t + 1).start()

        half = lax.rem(t, 2)
        wide_out[t] = stage[half].astype(f32).reshape(rows * groups, head_width)
        for g in range(groups):
            queries[g, t] = wide_out[t, pl.ds(g, rows, stride=groups)].astype(bf16)

    loop(blk_dev, spread)
    handed_on = [
        pltpu.make_async_copy(queries.at[groups - 1], query_out, misc_sem.at[6]),
        pltpu.make_async_copy(slot_map, slot_out, misc_sem.at[7]),
    ]
    for copy in handed_on:
        copy.start()

    @pl.when(level > 0)
    def _():
        early(0)

    def relay_keys(l):
        keys_up(l, l).wait_recv()
        keys_aside(l, core).start()

    def pair_keys(l):
        keys_aside(l, 1 - core).wait_recv()
        keys_across(l, col).start()

    def widen_keys(l):
        keys_across(l, 1 - col).wait_recv()
        for x in range(COLS):
            for c in range(CORES):
                summaries_wide[(l * COLS + x) * CORES + c] = summaries[l, x, c].astype(f32)

    loop(level, relay_keys)
    loop(level + 1, pair_keys)
    wanted_copy.wait_recv()
    local_wanted = pltpu.make_async_copy(peer_wanted, peer_wanted_s, misc_sem.at[3])
    local_wanted.start()
    local_wanted.wait()
    slots_copy.wait()
    loop(level + 1, widen_keys)

    def take(g, l):
        half = lax.rem(g, 2)
        aside(l, g, 1 - core).wait_recv()
        for c in range(CORES):
            first = (l * CORES + c) * blk_dev
            for b in range(blk_dev):
                cur[half, first + b] = column[l, c, g, b * block_len : (b + 1) * block_len]
        for c in range(CORES):
            source = (l * COLS + col) * CORES + c
            for k in range(CAP):
                index = peer_wanted_s[k, g, source * blk_dev]
                place = (c * CAP + k) * block_len
                peer_out[g, l, place : place + block_len] = cur[half, (l * CORES + c) * blk_dev + index]
        across(l, g).start()

        @pl.when(g == groups - 1)
        def _():
            pool_copy(0, l).start()

    def take_peer(g):
        half = lax.rem(g, 2)

        def body(i):
            l = level - i
            across(l, g).wait_recv()
            for k in range(picks):
                cur[half, slots_col + l * picks + k] = peer_in[g, l, k * block_len : (k + 1) * block_len]

            @pl.when(g == groups - 1)
            def _():
                pool_copy(1, l).start()

        loop(level + 1, body)

    factor = math.log2(math.e) * head_width ** (-0.5)
    across_lanes = (((1,), (1,)), ((), ()))

    def score_tile(t, first_group, groups_end):
        tile_number = rank * blk_dev + t
        seen = lax.broadcasted_iota(jnp.int32, (1, nblk), 1) <= tile_number

        def body(g):
            first = pl.multiple_of(g * blk_dev, blk_dev)
            summary = summaries_wide[:, pl.ds(first, blk_dev)].reshape(nblk, head_width).astype(bf16)
            logits = lax.dot_general(queries[g, t], summary, across_lanes, preferred_element_type=f32)
            logits = jnp.where(seen, logits, -jnp.inf)
            top = jnp.max(logits, axis=-1, keepdims=True)
            weights = jnp.exp2((logits - top) * factor)
            totals = jnp.sum(weights, axis=-1, keepdims=True)
            pooled = jnp.sum(weights / totals, axis=0, keepdims=True)
            pooled_ref[pl.ds(t * groups + g, 1), :] = pooled

        loop(groups_end, body, first_group)

    width = key_parts.shape[0]

    def attend(g, turn):
        half = lax.rem(g, 2)

        def unit(u):
            t = turn * width + u

            def store(start, count, result):
                wide_out[t, pl.ds(start * groups + g, count, stride=groups)] = result

            return (
                lambda place: pick_ref[t, g, place],
                lambda number: slot_map_s[g, number],
                rank * blk_dev + t,
                lambda here: queries[g, t, here],
                store,
            )

        work = (key_parts, value_parts, scores_parts, token_hot, mask_bank)
        attend_units(shape, cur.at[half], [unit(u) for u in range(width)], work)

    def put_out(t):
        @pl.when(t > 1)
        def _():
            out_copy(t - 2).wait()

        stage[lax.rem(t, 2)] = wide_out[t].reshape(rows, groups, head_width).astype(bf16)
        out_copy(t).start()

    def pool_copy(kind, l):
        count = (CORES * blk_dev, picks)[kind]
        here = pl.ds(kind * slots_col + l * count, count)
        return pltpu.make_async_copy(cur.at[(groups - 1) % 2, here], pool_out.at[here], pool_sem.at[kind, l])

    turns = blk_dev // width
    relay_at = [0] + [(i - 1) * (turns - 1) // max(levels - 2, 1) for i in range(1, levels)]
    take_at = [0] + [min(spot + 1, turns) for spot in relay_at[1:]]

    def relays(g, t, i):
        due = (t == relay_at[i]) & (level >= i)
        if i == 1:
            due = due & (g > 0) & (level == levels - 1)

        @pl.when(due)
        def _():
            relay(g, level - i)

        if i > 1:

            @pl.when((t == relay_at[i]) & (level == i) & (g + 1 >= lead) & (g + 1 < groups))
            def _():
                send_own(g + 1)

    def takes(g, t, i):
        @pl.when((t == take_at[i]) & (level >= i))
        def _():
            take(g, level - i)

    def main(g):
        def tiles(turn):
            for i in range(levels):
                if i > 0 and relay_at[i] < turns:
                    relays(g, turn, i)
                if take_at[i] < turns:
                    takes(g, turn, i)

            @pl.when(g > 0)
            def _():
                attend(g - 1, turn)

            @pl.when(g == groups - 1)
            def _():
                for u in range(width):
                    put_out(turn * width + u)

        loop(turns, tiles)
        for i in range(1, levels):
            if relay_at[i] == turns:
                relays(g, turns, i)

        @pl.when(has_above & (level > 0) & (g + 1 < groups))
        def _():
            early(g + 1)

        first_tile, end_tile = g * blk_dev // groups, (g + 1) * blk_dev // groups
        loop(end_tile, lambda t: score_tile(t, 0, groups // 2), first_tile)
        for i in range(1, levels):
            if take_at[i] == turns:
                takes(g, turns, i)
        loop(end_tile, lambda t: score_tile(t, groups // 2, groups), first_tile)
        take_peer(g)

    loop(groups, main)

    wanted_copy.wait_send()
    loop(levels, lambda l: keys_up(l, level).wait_send(), level + 1)

    def drain_keys(l):
        pool_copy(0, l).wait()
        pool_copy(1, l).wait()
        keys_aside(l, core).wait_send()
        keys_across(l, col).wait_send()

    loop(level + 1, drain_keys)

    def drain(g):
        def body(l):
            @pl.when(has_above)
            def _():
                up(l, g).wait_send()

            aside(l, g, core).wait_send()
            across(l, g).wait_send()

        loop(level + 1, body)

    loop(groups, drain)
    for t in range(max(blk_dev - 2, 0), blk_dev):
        out_copy(t).wait()
    for copy in handed_on:
        copy.wait()


def local(queries, key_rows, value_rows, compressed, chosen):
    _, tok_rows, heads_local, groups, head_width = queries.shape
    block_len = BLOCK
    shards = lax.axis_size("seq")
    blk_dev = tok_rows // block_len
    nblk = blk_dev * shards
    levels = shards // (COLS * CORES)
    rows = block_len * heads_local

    pick_rows = chosen[0]
    query_tiles = queries[0].reshape(blk_dev, rows, groups, head_width)
    shape = (levels, groups, blk_dev, heads_local, block_len, head_width)
    wide = 2 * head_width
    served = CORES * CAP * block_len
    part = min(rows, 256)
    width = 2 - blk_dev % 2
    dma = pltpu.SemaphoreType.DMA
    smem = pl.BlockSpec(memory_space=pltpu.SMEM)
    vmem = pl.BlockSpec(memory_space=pltpu.VMEM)
    anyspace = pl.BlockSpec(memory_space=pl.ANY)
    slots = levels * CORES * (blk_dev + CAP)
    bf16, f32 = jnp.bfloat16, jnp.float32
    partial, pooled, pool, last_queries, slot_map = pl.pallas_call(
        functools.partial(mega, shape),
        in_specs=[smem, vmem, vmem, anyspace, anyspace, anyspace],
        out_specs=[anyspace, vmem, anyspace, anyspace, anyspace],
        out_shape=[
            jax.ShapeDtypeStruct((blk_dev, rows, groups, head_width), bf16),
            jax.ShapeDtypeStruct((blk_dev * groups, nblk), f32),
            jax.ShapeDtypeStruct((slots, block_len, wide), bf16),
            jax.ShapeDtypeStruct((blk_dev, rows, head_width), bf16),
            jax.ShapeDtypeStruct((groups, nblk), jnp.int32),
        ],
        scratch_shapes=[
            pltpu.VMEM((levels, CORES, groups, tok_rows, wide), bf16),
            pltpu.VMEM((groups, levels, served, wide), bf16),
            pltpu.VMEM((groups, levels, served, wide), bf16),
            pltpu.VMEM((2, slots, block_len, wide), bf16),
            pltpu.VMEM((levels, COLS, CORES, groups * blk_dev, head_width), bf16),
            pltpu.VMEM((shards, groups * blk_dev, head_width), f32),
            pltpu.VMEM((groups, blk_dev, rows, head_width), bf16),
            pltpu.VMEM((blk_dev, rows * groups, head_width), f32),
            pltpu.VMEM((2, rows, groups, head_width), bf16),
            pltpu.VMEM((width, TOPN * block_len, wide), bf16),
            pltpu.VMEM((width, TOPN * block_len, wide), bf16),
            pltpu.VMEM((width, 2, part, TOPN * block_len), f32),
            pltpu.VMEM((rows, head_width), bf16),
            pltpu.VMEM((2, block_len, head_width), bf16),
            pltpu.VMEM((groups, nblk), jnp.int32),
            pltpu.SMEM((groups, nblk), jnp.int32),
            pltpu.VMEM((CAP, groups, nblk), jnp.int32),
            pltpu.VMEM((CAP, groups, nblk), jnp.int32),
            pltpu.SMEM((CAP, groups, nblk), jnp.int32),
        ]
        + [dma((levels, groups))] * 6
        + [dma((3, levels))] * 2
        + [dma((2,)), dma((2, levels)), dma((8,))],
        compiler_params=pltpu.CompilerParams(
            collective_id=0, has_side_effects=True, vmem_limit_bytes=67043328
        ),
    )(pick_rows, pick_rows, compressed[0], key_rows[0], value_rows[0], query_tiles)
    pooled = pooled.reshape(1, blk_dev, groups, nblk)
    shared = lax.psum_scatter(pooled, "head", scatter_dimension=2, tiled=True)
    groups_out = shared.shape[2]
    whole = pl.BlockSpec((slots, block_len, wide), lambda t: (0, 0, 0))
    lines = pl.BlockSpec((blk_dev * groups_out, nblk), lambda t: (0, 0))
    tile = pl.BlockSpec((width, rows, groups, head_width), lambda t: (t, 0, 0, 0))
    attended, block_scores = pl.pallas_call(
        functools.partial(finish, shape),
        grid=(blk_dev // width,),
        in_specs=[smem, smem, tile, pl.BlockSpec((width, rows, head_width), lambda t: (t, 0, 0)), whole, lines],
        out_specs=[tile, lines],
        out_shape=[
            jax.ShapeDtypeStruct((blk_dev, rows, groups, head_width), bf16),
            jax.ShapeDtypeStruct((blk_dev * groups_out, nblk), f32),
        ],
        scratch_shapes=[
            pltpu.VMEM((width, rows * groups, head_width), f32),
            pltpu.VMEM((width, TOPN * block_len, wide), bf16),
            pltpu.VMEM((width, TOPN * block_len, wide), bf16),
            pltpu.VMEM((width, 2, part, TOPN * block_len), f32),
            pltpu.VMEM((rows, head_width), bf16),
            pltpu.VMEM((2, block_len, head_width), bf16),
        ],
        compiler_params=pltpu.CompilerParams(
            dimension_semantics=("arbitrary",), vmem_limit_bytes=67043328
        ),
    )(pick_rows, slot_map, partial, last_queries, pool, shared.reshape(blk_dev * groups_out, nblk))
    block_scores = block_scores.reshape(1, blk_dev, groups_out, nblk)
    attended = attended.reshape(1, tok_rows, heads_local, groups, head_width)
    return (block_scores, attended)


def solution(mesh):
    placed = (
        P("batch", "seq", "head", None, None),
        P("batch", "seq", None, None),
        P("batch", "seq", None, None),
        P("batch", "seq", None, None),
        P("batch", "seq", None, None),
    )
    return jax.shard_map(
        local,
        mesh=mesh,
        in_specs=placed,
        out_specs=(P("batch", "seq", "head", None), P("batch", "seq", "head", None, None)),
        check_vma=False,
    )
```

```python
import functools
import math

import jax
import jax.numpy as jnp
from jax import lax
from jax.experimental import pallas as pl
from jax.experimental.pallas import tpu as pltpu
from jax.sharding import PartitionSpec as P

HPG = 8
BLOCK = 64
TOPN = 16
CAP = 2
COLS = 2
CORES = 2
MESH = pl.DeviceIdType.MESH


def prepare(shape, token_hot, mask_bank, value_parts):
    _, _, _, heads_local, block_len, head_width = shape
    rows = block_len * heads_local
    row_token = lax.broadcasted_iota(jnp.int32, (rows, head_width), 0) // heads_local
    row_lane = lax.broadcasted_iota(jnp.int32, (rows, head_width), 1)
    token_hot[...] = jnp.where(row_token == row_lane, 1.0, 0.0).astype(jnp.bfloat16)
    key_place = lax.broadcasted_iota(jnp.int32, (block_len, head_width), 0)
    key_lane = lax.broadcasted_iota(jnp.int32, (block_len, head_width), 1)
    mask_bank[0] = jnp.zeros((block_len, head_width), jnp.bfloat16)
    mask_bank[1] = jnp.where(key_place > key_lane, -1e30, 0.0).astype(jnp.bfloat16)
    lanes = value_parts.shape[2] - head_width
    for i in range(value_parts.shape[0]):
        value_parts[i, :, head_width:] = jnp.ones((TOPN * block_len, lanes), jnp.bfloat16)


def attend_units(shape, pool, units, work):
    _, _, _, heads_local, block_len, head_width = shape
    key_parts, value_parts, scores_parts, token_hot, mask_bank = work
    rows = block_len * heads_local
    part = min(rows, 256)
    parts = rows // part
    factor = math.log2(math.e) * head_width ** (-0.5)

    def gather(u):
        number_at, slot_at, tile_number, _, _ = units[u]
        for place in range(TOPN):
            here = slice(place * block_len, (place + 1) * block_len)
            number = number_at(place)
            slot = slot_at(number)
            is_own = (number == tile_number).astype(jnp.int32)
            key_parts[u, here, :head_width] = pool[slot, :, :head_width]
            key_parts[u, here, head_width:] = mask_bank[is_own]
            value_parts[u, here, :head_width] = pool[slot, :, head_width:]

    def score(u, i):
        here = pl.ds(i * part, part)
        query = jnp.concatenate([units[u][3](here), token_hot[here]], axis=1)
        scores_parts[u, i % 2] = lax.dot_general(
            query, key_parts[u], (((1,), (1,)), ((), ())), preferred_element_type=jnp.float32
        )

    def mix(u, i):
        scores = scores_parts[u, i % 2]
        top = jnp.max(scores, axis=-1, keepdims=True)
        weights = jnp.exp2((scores - top) * factor).astype(jnp.bfloat16)
        mixed = jnp.dot(weights, value_parts[u], preferred_element_type=jnp.float32)
        units[u][4](i * part, part, mixed[:, :head_width] / mixed[:, head_width:])

    steps = [(u, i) for u in range(len(units)) for i in range(parts)]
    gather(0)
    score(0, 0)
    for n, (u, i) in enumerate(steps):
        if n + 1 < len(steps):
            ahead = steps[n + 1]
            if i == 0 and u + 1 < len(units):
                gather(u + 1)
            score(*ahead)
        mix(u, i)


def finish(
    shape,
    pick_ref,
    slot_ref,
    partial_ref,
    query_ref,
    pool_ref,
    pooled_ref,
    out_ref,
    block_scores_ref,
    wide,
    key_parts,
    value_parts,
    scores_parts,
    token_hot,
    mask_bank,
):
    _, groups, blk_dev, heads_local, block_len, head_width = shape
    rows = block_len * heads_local
    rank = lax.axis_index("seq")
    step = pl.program_id(0)
    last = groups - 1
    width = wide.shape[0]

    @pl.when(step == 0)
    def _():
        prepare(shape, token_hot, mask_bank, value_parts)
        lines = pooled_ref.shape[0]
        line_tile = lax.broadcasted_iota(jnp.int32, (lines, 1), 0) // (lines // blk_dev)
        scale = (rank * blk_dev + line_tile + 1).astype(jnp.float32) / (block_len * HPG)
        block_scores_ref[...] = pooled_ref[...] * scale

    def unit(u):
        t = step * width + u

        def store(start, count, result):
            wide[u, pl.ds(start * groups + last, count, stride=groups)] = result

        return (
            lambda place: pick_ref[t, last, place],
            lambda number: slot_ref[last, number],
            rank * blk_dev + t,
            lambda here: query_ref[u, here],
            store,
        )

    for u in range(width):
        wide[u] = partial_ref[u].astype(jnp.float32).reshape(rows * groups, head_width)
    work = (key_parts, value_parts, scores_parts, token_hot, mask_bank)
    attend_units(shape, pool_ref, [unit(u) for u in range(width)], work)
    for u in range(width):
        out_ref[u] = wide[u].reshape(rows, groups, head_width).astype(jnp.bfloat16)


def mega(
    shape,
    pick_ref,
    chosen_ref,
    summary_ref,
    key_ref,
    value_ref,
    query_ref,
    out_ref,
    pooled_ref,
    pool_out,
    query_out,
    slot_out,
    column,
    peer_out,
    peer_in,
    cur,
    summaries,
    summaries_wide,
    queries,
    wide_out,
    stage,
    key_parts,
    value_parts,
    scores_parts,
    token_hot,
    mask_bank,
    slot_map,
    slot_map_s,
    wanted,
    peer_wanted,
    peer_wanted_s,
    up_send,
    up_recv,
    sib_send,
    sib_recv,
    peer_send,
    peer_recv,
    key_send,
    key_recv,
    stage_sem,
    pool_sem,
    misc_sem,
):
    levels, groups, blk_dev, heads_local, block_len, head_width = shape
    rows = block_len * heads_local
    tokens = blk_dev * block_len
    per_level = COLS * CORES
    nblk = levels * per_level * blk_dev
    slots_col = levels * CORES * blk_dev
    picks = CORES * CAP
    f32, bf16 = jnp.float32, jnp.bfloat16

    rank = lax.axis_index("seq")
    core = lax.rem(rank, CORES)
    col = lax.rem(rank // CORES, COLS)
    level = rank // per_level
    sibling = rank + 1 - 2 * core
    peer = rank + CORES * (1 - 2 * col)
    above = rank + per_level
    has_above = level < levels - 1

    def loop(n, body, start=0):
        def step(i, carry):
            body(i)
            return carry

        lax.fori_loop(start, n, step, 0)

    barrier = pltpu.get_barrier_semaphore()
    for other in (sibling, peer):
        pl.semaphore_signal(barrier, inc=1, device_id={"seq": other}, device_id_type=MESH)
    for step in range(1, levels):
        other = lax.rem(rank + step * per_level, levels * per_level)
        pl.semaphore_signal(barrier, inc=1, device_id={"seq": other}, device_id_type=MESH)

    def query_copy(t):
        half = lax.rem(t, 2)
        return pltpu.make_async_copy(query_ref.at[t], stage.at[half], stage_sem.at[half])

    def out_copy(t):
        half = lax.rem(t, 2)
        return pltpu.make_async_copy(stage.at[half], out_ref.at[t], stage_sem.at[half])

    def remote(src, dst, send, recv, device):
        return pltpu.make_async_remote_copy(
            src, dst, send, recv, device_id={"seq": device}, device_id_type=MESH
        )

    def up(l, g):
        part = column.at[l, core, g]
        return remote(part, part, up_send.at[l, g], up_recv.at[l, g], above)

    def aside(l, g, owner):
        part = column.at[l, owner, g]
        return remote(part, part, sib_send.at[l, g], sib_recv.at[l, g], sibling)

    def across(l, g):
        return remote(peer_out.at[g, l], peer_in.at[g, l], peer_send.at[l, g], peer_recv.at[l, g], peer)

    def keys_up(l, source):
        part = summaries.at[source, col, core]
        return remote(part, part, key_send.at[0, l], key_recv.at[0, source], rank + (l - level) * per_level)

    def keys_aside(l, owner):
        part = summaries.at[l, col, owner]
        return remote(part, part, key_send.at[1, l], key_recv.at[1, l], sibling)

    def keys_across(l, owner):
        part = summaries.at[l, owner]
        return remote(part, part, key_send.at[2, l], key_recv.at[2, l], peer)

    wanted_copy = remote(wanted, peer_wanted, misc_sem.at[0], misc_sem.at[1], peer)
    slots_copy = pltpu.make_async_copy(slot_map, slot_map_s, misc_sem.at[2])
    def load(slab, kind, ref):
        return pltpu.make_async_copy(
            ref.at[slab * rows : (slab + 1) * rows], stage.at[kind], misc_sem.at[4 + kind]
        )

    load(0, 0, key_ref).start()
    load(0, 1, value_ref).start()

    own_summary = jnp.swapaxes(summary_ref[...].astype(f32), 0, 1)
    own_summary = own_summary.reshape(groups * blk_dev, head_width).astype(bf16)
    summaries[level, col, core] = own_summary
    for slab in range(tokens // rows):
        for kind, ref in enumerate((key_ref, value_ref)):
            load(slab, kind, ref).wait()

            def split(r, slab=slab, kind=kind):
                source = pl.ds(pl.multiple_of(r * block_len, block_len), block_len)
                place = pl.multiple_of(slab * rows + r * block_len, block_len)
                apart = jnp.swapaxes(stage[kind, source].astype(f32), 0, 1).astype(bf16)
                lanes = slice(kind * head_width, (kind + 1) * head_width)
                for g in range(groups):
                    column[level, core, g, pl.ds(place, block_len), lanes] = apart[g]

            loop(heads_local, split)
            if (slab + 1) * rows < tokens:
                load(slab + 1, kind, ref).start()
    query_copy(0).start()
    pl.semaphore_wait(barrier, levels + 1)

    loop(levels, lambda l: keys_up(l, level).start(), level + 1)
    keys_aside(level, core).start()

    def send_own(g):
        @pl.when(has_above)
        def _():
            up(level, g).start()

    lead = jnp.where(level == 0, groups, jnp.where(level == levels - 2, min(3, groups), 1))
    loop(lead, send_own)
    loop(groups, lambda g: aside(level, g, core).start())

    number = lax.broadcasted_iota(jnp.int32, (groups, nblk), 1)
    named = jnp.zeros((groups, nblk), jnp.int32)
    for t in range(blk_dev):
        picks_here = chosen_ref[t]
        for place in range(TOPN):
            named = jnp.where(picks_here[:, place : place + 1] == number, 1, named)
    inside = lax.rem(number, blk_dev)
    order = named
    step = 1
    while step < blk_dev:
        order = order + jnp.where(inside >= step, pltpu.roll(order, step, 1), 0)
        step *= 2
    order = order - named
    for k in range(CAP):
        found = jnp.where((named == 1) & (order == k), inside, 0)
        step = 1
        while step < blk_dev:
            found = found + pltpu.roll(found, nblk - step, 1)
            step *= 2
        wanted[k] = found
    device = number // blk_dev
    pair = device // per_level * CORES + lax.rem(device, CORES)
    in_column = lax.rem(device // CORES, COLS) == col
    slot_map[...] = jnp.where(in_column, pair * blk_dev + inside, slots_col + pair * CAP + order)

    prepare(shape, token_hot, mask_bank, value_parts)
    summaries_wide[...] = jnp.zeros_like(summaries_wide)
    wanted_copy.start()
    slots_copy.start()

    def relay(g, l):
        up(l, g).wait_recv()

        @pl.when(has_above)
        def _():
            up(l, g).start()

        aside(l, g, core).start()

    def early(g):
        relay(g, level - 1)

        @pl.when((level == 1) & (g + 1 >= lead) & (g + 1 < groups))
        def _():
            send_own(g + 1)

    def spread(t):
        query_copy(t).wait()

        @pl.when(t + 1 < blk_dev)
        def _():
            query_copy(t + 1).start()

        half = lax.rem(t, 2)
        wide_out[t] = stage[half].astype(f32).reshape(rows * groups, head_width)
        for g in range(groups):
            queries[g, t] = wide_out[t, pl.ds(g, rows, stride=groups)].astype(bf16)

    loop(blk_dev, spread)
    handed_on = [
        pltpu.make_async_copy(queries.at[groups - 1], query_out, misc_sem.at[6]),
        pltpu.make_async_copy(slot_map, slot_out, misc_sem.at[7]),
    ]
    for copy in handed_on:
        copy.start()

    @pl.when(level > 0)
    def _():
        early(0)

    def relay_keys(l):
        keys_up(l, l).wait_recv()
        keys_aside(l, core).start()

    def pair_keys(l):
        keys_aside(l, 1 - core).wait_recv()
        keys_across(l, col).start()

    def widen_keys(l):
        keys_across(l, 1 - col).wait_recv()
        for x in range(COLS):
            for c in range(CORES):
                summaries_wide[(l * COLS + x) * CORES + c] = summaries[l, x, c].astype(f32)

    loop(level, relay_keys)
    loop(level + 1, pair_keys)
    wanted_copy.wait_recv()
    local_wanted = pltpu.make_async_copy(peer_wanted, peer_wanted_s, misc_sem.at[3])
    local_wanted.start()
    local_wanted.wait()
    slots_copy.wait()
    loop(level + 1, widen_keys)

    def take(g, l):
        half = lax.rem(g, 2)
        aside(l, g, 1 - core).wait_recv()
        for c in range(CORES):
            first = (l * CORES + c) * blk_dev
            for b in range(blk_dev):
                cur[half, first + b] = column[l, c, g, b * block_len : (b + 1) * block_len]
        for c in range(CORES):
            source = (l * COLS + col) * CORES + c
            for k in range(CAP):
                index = peer_wanted_s[k, g, source * blk_dev]
                place = (c * CAP + k) * block_len
                peer_out[g, l, place : place + block_len] = cur[half, (l * CORES + c) * blk_dev + index]
        across(l, g).start()

        @pl.when(g == groups - 1)
        def _():
            pool_copy(0, l).start()

    def take_peer(g):
        half = lax.rem(g, 2)

        def body(i):
            l = level - i
            across(l, g).wait_recv()
            for k in range(picks):
                cur[half, slots_col + l * picks + k] = peer_in[g, l, k * block_len : (k + 1) * block_len]

            @pl.when(g == groups - 1)
            def _():
                pool_copy(1, l).start()

        loop(level + 1, body)

    factor = math.log2(math.e) * head_width ** (-0.5)
    across_lanes = (((1,), (1,)), ((), ()))

    def score_tile(t, first_group, groups_end):
        tile_number = rank * blk_dev + t
        seen = lax.broadcasted_iota(jnp.int32, (1, nblk), 1) <= tile_number

        def body(g):
            first = pl.multiple_of(g * blk_dev, blk_dev)
            summary = summaries_wide[:, pl.ds(first, blk_dev)].reshape(nblk, head_width).astype(bf16)
            logits = lax.dot_general(queries[g, t], summary, across_lanes, preferred_element_type=f32)
            logits = jnp.where(seen, logits, -jnp.inf)
            top = jnp.max(logits, axis=-1, keepdims=True)
            weights = jnp.exp2((logits - top) * factor)
            totals = jnp.sum(weights, axis=-1, keepdims=True)
            pooled = jnp.sum(weights / totals, axis=0, keepdims=True)
            pooled_ref[pl.ds(t * groups + g, 1), :] = pooled

        loop(groups_end, body, first_group)

    width = key_parts.shape[0]

    def attend(g, turn):
        half = lax.rem(g, 2)

        def unit(u):
            t = turn * width + u

            def store(start, count, result):
                wide_out[t, pl.ds(start * groups + g, count, stride=groups)] = result

            return (
                lambda place: pick_ref[t, g, place],
                lambda number: slot_map_s[g, number],
                rank * blk_dev + t,
                lambda here: queries[g, t, here],
                store,
            )

        work = (key_parts, value_parts, scores_parts, token_hot, mask_bank)
        attend_units(shape, cur.at[half], [unit(u) for u in range(width)], work)

    def put_out(t):
        @pl.when(t > 1)
        def _():
            out_copy(t - 2).wait()

        stage[lax.rem(t, 2)] = wide_out[t].reshape(rows, groups, head_width).astype(bf16)
        out_copy(t).start()

    def pool_copy(kind, l):
        count = (CORES * blk_dev, picks)[kind]
        here = pl.ds(kind * slots_col + l * count, count)
        return pltpu.make_async_copy(cur.at[(groups - 1) % 2, here], pool_out.at[here], pool_sem.at[kind, l])

    turns = blk_dev // width
    relay_at = [0] + [(i - 1) * (turns - 1) // max(levels - 2, 1) for i in range(1, levels)]
    take_at = [0] + [min(spot + 1, turns) for spot in relay_at[1:]]

    def relays(g, t, i):
        due = (t == relay_at[i]) & (level >= i)
        if i == 1:
            due = due & (g > 0) & (level == levels - 1)

        @pl.when(due)
        def _():
            relay(g, level - i)

        if i > 1:

            @pl.when((t == relay_at[i]) & (level == i) & (g + 1 >= lead) & (g + 1 < groups))
            def _():
                send_own(g + 1)

    def takes(g, t, i):
        @pl.when((t == take_at[i]) & (level >= i))
        def _():
            take(g, level - i)

    def main(g):
        def tiles(turn):
            for i in range(levels):
                if i > 0 and relay_at[i] < turns:
                    relays(g, turn, i)
                if take_at[i] < turns:
                    takes(g, turn, i)

            @pl.when(g > 0)
            def _():
                attend(g - 1, turn)

            @pl.when(g == groups - 1)
            def _():
                for u in range(width):
                    put_out(turn * width + u)

        loop(turns, tiles)
        for i in range(1, levels):
            if relay_at[i] == turns:
                relays(g, turns, i)

        @pl.when(has_above & (level > 0) & (g + 1 < groups))
        def _():
            early(g + 1)

        first_tile, end_tile = g * blk_dev // groups, (g + 1) * blk_dev // groups
        for i in range(1, levels):
            if take_at[i] == turns:
                takes(g, turns, i)
        loop(end_tile, lambda t: score_tile(t, 0, groups), first_tile)
        take_peer(g)

    loop(groups, main)

    wanted_copy.wait_send()
    loop(levels, lambda l: keys_up(l, level).wait_send(), level + 1)

    def drain_keys(l):
        pool_copy(0, l).wait()
        pool_copy(1, l).wait()
        keys_aside(l, core).wait_send()
        keys_across(l, col).wait_send()

    loop(level + 1, drain_keys)

    def drain(g):
        def body(l):
            @pl.when(has_above)
            def _():
                up(l, g).wait_send()

            aside(l, g, core).wait_send()
            across(l, g).wait_send()

        loop(level + 1, body)

    loop(groups, drain)
    for t in range(max(blk_dev - 2, 0), blk_dev):
        out_copy(t).wait()
    for copy in handed_on:
        copy.wait()


def local(queries, key_rows, value_rows, compressed, chosen):
    _, tok_rows, heads_local, groups, head_width = queries.shape
    block_len = BLOCK
    shards = lax.axis_size("seq")
    blk_dev = tok_rows // block_len
    nblk = blk_dev * shards
    levels = shards // (COLS * CORES)
    rows = block_len * heads_local

    pick_rows = chosen[0]
    query_tiles = queries[0].reshape(blk_dev, rows, groups, head_width)
    shape = (levels, groups, blk_dev, heads_local, block_len, head_width)
    wide = 2 * head_width
    served = CORES * CAP * block_len
    part = min(rows, 256)
    width = 2 - blk_dev % 2
    dma = pltpu.SemaphoreType.DMA
    smem = pl.BlockSpec(memory_space=pltpu.SMEM)
    vmem = pl.BlockSpec(memory_space=pltpu.VMEM)
    anyspace = pl.BlockSpec(memory_space=pl.ANY)
    slots = levels * CORES * (blk_dev + CAP)
    bf16, f32 = jnp.bfloat16, jnp.float32
    partial, pooled, pool, last_queries, slot_map = pl.pallas_call(
        functools.partial(mega, shape),
        in_specs=[smem, vmem, vmem, anyspace, anyspace, anyspace],
        out_specs=[anyspace, vmem, anyspace, anyspace, anyspace],
        out_shape=[
            jax.ShapeDtypeStruct((blk_dev, rows, groups, head_width), bf16),
            jax.ShapeDtypeStruct((blk_dev * groups, nblk), f32),
            jax.ShapeDtypeStruct((slots, block_len, wide), bf16),
            jax.ShapeDtypeStruct((blk_dev, rows, head_width), bf16),
            jax.ShapeDtypeStruct((groups, nblk), jnp.int32),
        ],
        scratch_shapes=[
            pltpu.VMEM((levels, CORES, groups, tok_rows, wide), bf16),
            pltpu.VMEM((groups, levels, served, wide), bf16),
            pltpu.VMEM((groups, levels, served, wide), bf16),
            pltpu.VMEM((2, slots, block_len, wide), bf16),
            pltpu.VMEM((levels, COLS, CORES, groups * blk_dev, head_width), bf16),
            pltpu.VMEM((shards, groups * blk_dev, head_width), f32),
            pltpu.VMEM((groups, blk_dev, rows, head_width), bf16),
            pltpu.VMEM((blk_dev, rows * groups, head_width), f32),
            pltpu.VMEM((2, rows, groups, head_width), bf16),
            pltpu.VMEM((width, TOPN * block_len, wide), bf16),
            pltpu.VMEM((width, TOPN * block_len, wide), bf16),
            pltpu.VMEM((width, 2, part, TOPN * block_len), f32),
            pltpu.VMEM((rows, head_width), bf16),
            pltpu.VMEM((2, block_len, head_width), bf16),
            pltpu.VMEM((groups, nblk), jnp.int32),
            pltpu.SMEM((groups, nblk), jnp.int32),
            pltpu.VMEM((CAP, groups, nblk), jnp.int32),
            pltpu.VMEM((CAP, groups, nblk), jnp.int32),
            pltpu.SMEM((CAP, groups, nblk), jnp.int32),
        ]
        + [dma((levels, groups))] * 6
        + [dma((3, levels))] * 2
        + [dma((2,)), dma((2, levels)), dma((8,))],
        compiler_params=pltpu.CompilerParams(
            collective_id=0, has_side_effects=True, vmem_limit_bytes=67043328
        ),
    )(pick_rows, pick_rows, compressed[0], key_rows[0], value_rows[0], query_tiles)
    pooled = pooled.reshape(1, blk_dev, groups, nblk)
    shared = lax.psum_scatter(pooled, "head", scatter_dimension=2, tiled=True)
    groups_out = shared.shape[2]
    whole = pl.BlockSpec((slots, block_len, wide), lambda t: (0, 0, 0))
    lines = pl.BlockSpec((blk_dev * groups_out, nblk), lambda t: (0, 0))
    tile = pl.BlockSpec((width, rows, groups, head_width), lambda t: (t, 0, 0, 0))
    attended, block_scores = pl.pallas_call(
        functools.partial(finish, shape),
        grid=(blk_dev // width,),
        in_specs=[smem, smem, tile, pl.BlockSpec((width, rows, head_width), lambda t: (t, 0, 0)), whole, lines],
        out_specs=[tile, lines],
        out_shape=[
            jax.ShapeDtypeStruct((blk_dev, rows, groups, head_width), bf16),
            jax.ShapeDtypeStruct((blk_dev * groups_out, nblk), f32),
        ],
        scratch_shapes=[
            pltpu.VMEM((width, rows * groups, head_width), f32),
            pltpu.VMEM((width, TOPN * block_len, wide), bf16),
            pltpu.VMEM((width, TOPN * block_len, wide), bf16),
            pltpu.VMEM((width, 2, part, TOPN * block_len), f32),
            pltpu.VMEM((rows, head_width), bf16),
            pltpu.VMEM((2, block_len, head_width), bf16),
        ],
        compiler_params=pltpu.CompilerParams(
            dimension_semantics=("arbitrary",), vmem_limit_bytes=67043328
        ),
    )(pick_rows, slot_map, partial, last_queries, pool, shared.reshape(blk_dev * groups_out, nblk))
    block_scores = block_scores.reshape(1, blk_dev, groups_out, nblk)
    attended = attended.reshape(1, tok_rows, heads_local, groups, head_width)
    return (block_scores, attended)


def solution(mesh):
    placed = (
        P("batch", "seq", "head", None, None),
        P("batch", "seq", None, None),
        P("batch", "seq", None, None),
        P("batch", "seq", None, None),
        P("batch", "seq", None, None),
    )
    return jax.shard_map(
        local,
        mesh=mesh,
        in_specs=placed,
        out_specs=(P("batch", "seq", "head", None), P("batch", "seq", "head", None, None)),
        check_vma=False,
    )
```
